16 devices in a mesh: dp: 4 (over z, y), ep: 4 (over x, core).
Axes of the slice: x: 2, y: 2, z: 2, core: 2. Of those that a mesh axis runs over, the one named last changes fastest.
Arguments:
- x_rows: bfloat16 [512, 1024], P(('dp', 'ep')), parts along dimension 0
- expert_idx: int32 [512, 8], P(('dp', 'ep')), parts along dimension 0
- gate_w: float32 [512, 8], P(('dp', 'ep')), parts along dimension 0
- slot_pos: int32 [512, 8], P(('dp', 'ep')), parts along dimension 0
- w_gate: bfloat16 [32, 1024, 512], P('ep')
- w_up: bfloat16 [32, 1024, 512], P('ep')
- w_down: bfloat16 [32, 512, 1024], P('ep')
- grad_out: bfloat16 [512, 1024], P(('dp', 'ep')), parts along dimension 0
Outputs:
- output 1: bfloat16 [512, 1024], P(('dp', 'ep')), parts along dimension 0
- output 2: bfloat16 [512, 1024], P(('dp', 'ep')), parts along dimension 0
- output 3: bfloat16 [128, 1024, 512], P(('dp', 'ep')), parts along dimension 0
- output 4: bfloat16 [128, 1024, 512], P(('dp', 'ep')), parts along dimension 0
- output 5: bfloat16 [128, 512, 1024], P(('dp', 'ep')), parts along dimension 0
- output 6: float32 [512, 8], P(('dp', 'ep')), parts along dimension 0
There are 4 independent parts. The reference program is written for one: setup_inputs(seed, part) draws one part's arguments, and reference() takes and returns one part's arrays. A program takes and returns all parts, laid end to end along the dimension named above; an argument that names none is the same for every part.
All inputs are finite; a program needn't handle non-finite values.
Results may differ from the reference program's by a relative error of at most 0.0103458.
Values are sent between devices in bfloat16 or wider.
A program may use at most 1 GiB of HBM per device.

```python
import jax
import jax.numpy as jnp
from jax import lax

TOK = 32
D = 1024
FF = 512
EXPERTS = 32
TOP = 8
GROUP = 4

CAP = ((2 * TOK * TOP + EXPERTS - 1) // EXPERTS + 7) // 8 * 8
HOT_ROWS = CAP + CAP // 4
TOKENS = GROUP * TOK
CHOICES = TOK * TOP
ROWS = EXPERTS * CAP


def rank_in_expert(expert_list):
    sort_order = jnp.argsort(expert_list, stable=True)
    ordered = expert_list[sort_order]
    first_pos = jnp.searchsorted(ordered, ordered)
    rank_sorted = (jnp.arange(CHOICES) - first_pos).astype(jnp.int32)
    return jnp.zeros((CHOICES,), jnp.int32).at[sort_order].set(rank_sorted)


def draw_routing(route_key):
    key_hot, key_rank, key_score = jax.random.split(route_key, 3)
    hot_expert = jax.random.randint(key_hot, (GROUP, 1, 1), 0, EXPERTS)
    tok_rank = jax.vmap(lambda sub_key: jax.random.permutation(sub_key, TOK))(jax.random.split(key_rank, GROUP))
    is_hot = (tok_rank < HOT_ROWS)[:, :, None]
    expert_ids = jnp.arange(EXPERTS, dtype=jnp.int32)
    base_score = jax.random.randint(key_score, (GROUP, TOK, EXPERTS), 0, 2 ** 20)
    hot_bonus = jnp.where(is_hot & (expert_ids == hot_expert), 2 ** 21, 0)
    score_int = (base_score + hot_bonus) * EXPERTS + expert_ids
    chosen = jnp.argsort(-score_int, axis=-1)[:, :, :TOP].astype(jnp.int32)
    rank_all = jax.vmap(rank_in_expert)(chosen.reshape(GROUP, CHOICES))
    slot_all = jnp.where(rank_all < CAP, rank_all, -1).astype(jnp.int32)
    return chosen.reshape(TOKENS, TOP), slot_all.reshape(TOKENS, TOP)


def setup_inputs(seed: int = 0, part: int = 0) -> dict:
    root_key = jax.random.key(seed)
    shared_key, data_key = jax.random.split(root_key)
    part_key = jax.random.fold_in(data_key, part)
    key_route, key_x, key_gate, key_grad = jax.random.split(part_key, 4)
    key_wg, key_wu, key_wd = jax.random.split(shared_key, 3)
    expert_idx, slot_pos = draw_routing(key_route)
    x_rows = jax.random.normal(key_x, (TOKENS, D), jnp.float32).astype(jnp.bfloat16)
    gate_w = jax.random.uniform(key_gate, (TOKENS, TOP), jnp.float32, 0.5, 1.5) * TOP ** -0.5
    w_gate = (jax.random.normal(key_wg, (EXPERTS, D, FF), jnp.float32) * D ** -0.5).astype(jnp.bfloat16)
    w_up = (jax.random.normal(key_wu, (EXPERTS, D, FF), jnp.float32) * D ** -0.5).astype(jnp.bfloat16)
    w_down = (jax.random.normal(key_wd, (EXPERTS, FF, D), jnp.float32) * FF ** -0.5).astype(jnp.bfloat16)
    grad_out = jax.random.normal(key_grad, (TOKENS, D), jnp.float32).astype(jnp.bfloat16)
    return {'x_rows': x_rows, 'expert_idx': expert_idx, 'gate_w': gate_w, 'slot_pos': slot_pos, 'w_gate': w_gate, 'w_up': w_up, 'w_down': w_down, 'grad_out': grad_out}


def take_rows(table, where_from):
    return jnp.take(table, where_from, axis=0, mode='fill', fill_value=0)


def to_experts(dev_rows):
    return dev_rows.reshape(GROUP, EXPERTS, CAP, D).transpose(1, 0, 2, 3).reshape(EXPERTS, GROUP * CAP, D)


def to_devices(exp_rows):
    return exp_rows.reshape(EXPERTS, GROUP, CAP, D).transpose(1, 0, 2, 3).reshape(GROUP, ROWS, D)


def expert_pass(operands):
    in_rows, dy_rows, gate_mat, up_mat, down_mat = operands
    pre_gate = jnp.dot(in_rows, gate_mat, preferred_element_type=jnp.float32)
    pre_up = jnp.dot(in_rows, up_mat, preferred_element_type=jnp.float32)
    gate_sig = jax.nn.sigmoid(pre_gate)
    gate_act = pre_gate * gate_sig
    hidden = (gate_act * pre_up).astype(jnp.bfloat16)
    out_exp = jnp.dot(hidden, down_mat, preferred_element_type=jnp.float32).astype(jnp.bfloat16)
    d_hidden = jnp.dot(dy_rows, down_mat.T, preferred_element_type=jnp.float32)
    d_gate = (d_hidden * pre_up * (gate_sig * (1.0 + pre_gate * (1.0 - gate_sig)))).astype(jnp.bfloat16)
    d_up = (d_hidden * gate_act).astype(jnp.bfloat16)
    g_down = jnp.dot(hidden.T, dy_rows, preferred_element_type=jnp.float32).astype(jnp.bfloat16)
    g_gate = jnp.dot(in_rows.T, d_gate, preferred_element_type=jnp.float32).astype(jnp.bfloat16)
    g_up = jnp.dot(in_rows.T, d_up, preferred_element_type=jnp.float32).astype(jnp.bfloat16)
    d_in = (jnp.dot(d_gate, gate_mat.T, preferred_element_type=jnp.float32) + jnp.dot(d_up, up_mat.T, preferred_element_type=jnp.float32)).astype(jnp.bfloat16)
    return out_exp, d_in, g_gate, g_up, g_down


def reference(x_rows, expert_idx, gate_w, slot_pos, w_gate, w_up, w_down, grad_out):
    flat_pos = jnp.where(slot_pos >= 0, expert_idx * CAP + slot_pos, ROWS).reshape(GROUP, CHOICES)
    choice_ids = jnp.arange(CHOICES, dtype=jnp.int32)
    src_choice = jax.vmap(lambda pos_row: jnp.full((ROWS,), CHOICES, jnp.int32).at[pos_row].set(choice_ids, mode='drop'))(flat_pos)
    src_tok = src_choice // TOP
    rows_of = jax.vmap(take_rows)
    sent_x = rows_of(x_rows.reshape(GROUP, TOK, D), src_tok)
    w_rows = rows_of(gate_w.reshape(GROUP, CHOICES), src_choice)
    g_rows = rows_of(grad_out.reshape(GROUP, TOK, D), src_tok)
    sent_dy = (w_rows[:, :, None] * g_rows.astype(jnp.float32)).astype(jnp.bfloat16)
    out_exp, d_in, grad_w_gate, grad_w_up, grad_w_down = lax.map(expert_pass, (to_experts(sent_x), to_experts(sent_dy), w_gate, w_up, w_down))
    y_choice = rows_of(to_devices(out_exp), flat_pos).reshape(TOKENS, TOP, D)
    d_choice = rows_of(to_devices(d_in), flat_pos).reshape(TOKENS, TOP, D)
    out_rows = jnp.sum(gate_w[:, :, None] * y_choice.astype(jnp.float32), axis=1).astype(jnp.bfloat16)
    grad_x = jnp.sum(d_choice.astype(jnp.float32), axis=1).astype(jnp.bfloat16)
    grad_gate = jnp.sum(grad_out[:, None, :].astype(jnp.float32) * y_choice.astype(jnp.float32), axis=-1)
    return out_rows, grad_x, grad_w_gate, grad_w_up, grad_w_down, grad_gate
```

```python
import functools

import jax
import jax.numpy as jnp
from jax import lax
from jax.experimental import pallas as pl
from jax.experimental.pallas import tpu as pltpu
from jax.sharding import PartitionSpec as P

F32 = jnp.float32
BF16 = jnp.bfloat16
MESH = pl.DeviceIdType.MESH
LANE = 128
NT = (((1,), (1,)), ((), ()))


def dot(a, b):
    return jnp.dot(a, b, preferred_element_type=F32)


def dot_nt(a, b):
    return lax.dot_general(a, b, NT, preferred_element_type=F32)


def forward_kernel(n, idx_h, gate_h, slot_h, x_h, g_h, w1_h, w3_h, w2_h,
                   w1, w3, w2, gg, gb, mb, hT, pf, qf, xT, own, s1, s2, s3,
                   xg, idx_v, gate_v, slot_v, h_v, acc,
                   load_sem, w_sem, send_sem, recv_sem):
    me = lax.axis_index("ep")
    sib, opp = lax.bitwise_xor(me, 1), lax.bitwise_xor(me, 2)
    n_local = w1.shape[0]
    tok, model = x_h.shape
    ffn = w1.shape[2]
    n_tok = n * tok

    barrier = pltpu.get_barrier_semaphore()
    for other in (sib, opp):
        pl.semaphore_signal(barrier, inc=1, device_id={"ep": other}, device_id_type=MESH)

    srcs = (idx_h, gate_h, slot_h, x_h, g_h)
    bufs = (idx_v, gate_v, slot_v, xg, gg)
    loads = [pltpu.make_async_copy(s, b.at[me], load_sem.at[i]) for i, (s, b) in enumerate(zip(srcs, bufs))]
    for c in loads:
        c.start()

    def w_copy(k, e):
        wh, wv = ((w1_h, w1), (w3_h, w3), (w2_h, w2))[k]
        return pltpu.make_async_copy(wh.at[e], wv.at[e], w_sem.at[k, e])

    for e in range(n_local):
        w_copy(0, e).start()
        w_copy(1, e).start()
    for e in range(n_local):
        w_copy(2, e).start()

    def send(i, block, to, k):
        return pltpu.make_async_remote_copy(
            src_ref=bufs[i].at[block], dst_ref=bufs[i].at[block],
            send_sem=send_sem.at[i, k], recv_sem=recv_sem.at[i, k],
            device_id={"ep": to}, device_id_type=MESH)

    for c in loads[:4]:
        c.wait()
    pl.semaphore_wait(barrier, 2)
    to_opp = [send(i, me, opp, 0) for i in range(5)]
    to_sib = [send(i, me, sib, 1) for i in range(5)]
    relay = [send(i, opp, sib, 2) for i in range(5)]
    for i in range(4):
        to_opp[i].start()
        to_sib[i].start()
    loads[4].wait()
    to_opp[4].start()
    to_sib[4].start()
    for i in range(4):
        to_opp[i].wait_recv()
        relay[i].start()
    for i in range(4):
        to_sib[i].wait_recv()
        relay[i].wait_recv()

    def rows_of(buf):
        return jnp.concatenate([buf[b] for b in range(n)], axis=1).T

    lane = lax.broadcasted_iota(jnp.int32, (n_tok, LANE), 1)
    ib, gt, sl = rows_of(idx_v), rows_of(gate_v), rows_of(slot_v)
    gd = jnp.zeros((n_tok, LANE), F32)
    md = jnp.zeros((n_tok, LANE), F32)
    for j in range(ib.shape[1]):
        hit = (ib[:, j:j + 1] == lane + me * n_local) & (sl[:, j:j + 1] >= 0)
        gd = jnp.where(hit, gt[:, j:j + 1], gd)
        md = jnp.where(hit, 1.0, md)
    for e in range(n_local):
        gb[e] = jnp.broadcast_to(gd[:, e:e + 1], (n_tok, LANE))
        mb[e] = jnp.broadcast_to(md[:, e:e + 1], (n_tok, LANE))

    x = xg[...].reshape(n_tok, model)
    xT[...] = x.T

    half = 256

    def up(e, _):
        w_copy(0, e).wait()
        w_copy(1, e).wait()
        keep = mb[e] > 0.0
        keep = jnp.concatenate([keep, keep], axis=1)
        for c in range(ffn // half):
            col = slice(c * half, (c + 1) * half)
            xv = xg[...].reshape(n_tok, model)
            a = dot(xv, w1[e, :, col])
            b = dot(xv, w3[e, :, col])
            sg = jax.nn.sigmoid(a)
            ga = a * sg
            h = jnp.where(keep, ga * b, 0.0).astype(BF16)
            h_v[e, :, col] = h
            hT[e, col, :] = h.T
            pf[e, :, col] = b * (sg * (1.0 + a * (1.0 - sg)))
            qf[e, :, col] = ga
        return 0

    lax.fori_loop(0, n_local // 2, up, 0, unroll=2)
    to_opp[4].wait_recv()
    relay[4].start()
    lax.fori_loop(n_local // 2, n_local, up, 0, unroll=2)
    to_sib[4].wait_recv()
    relay[4].wait_recv()

    acc[...] = jnp.zeros_like(acc)
    lane_all = lax.broadcasted_iota(jnp.int32, (n_tok, LANE), 1)

    def down(e, _):
        w_copy(2, e).wait()
        hv = h_v[e]
        gv = gb[e]
        part = jnp.zeros((n_tok, LANE), F32)
        for c in range(model // half):
            y = dot(hv, w2[e, :, c * half:(c + 1) * half]).astype(BF16).astype(F32)
            for k in range(half // LANE):
                yk = y[:, k * LANE:(k + 1) * LANE]
                col = slice(c * half + k * LANE, c * half + (k + 1) * LANE)
                acc[:, col] += gv * yk
                part += gg[:, :, col].reshape(n_tok, LANE).astype(F32) * yk
        row = jnp.sum(part, axis=1, keepdims=True)
        acc[:, model:] += jnp.where(lane_all == me * n_local + e, row, 0.0)
        return 0

    lax.fori_loop(0, n_local, down, 0, unroll=2)
    for k, o in enumerate((own, s1, s2, s3)):
        blk = lax.bitwise_xor(me, k)
        o[...] = acc[pl.ds(pl.multiple_of(blk * tok, tok), tok), :]

    for i in range(5):
        to_opp[i].wait_send()
        to_sib[i].wait_send()
        relay[i].wait_send()


def dgrad_kernel(n, w1, w3, w2, gg, gb, mb, hT, pf, qf, gwd_h, da_o, db_o, own, s1, s2, s3,
                 dy, acc, stage, sem):
    me = lax.axis_index("ep")
    n_local = w1.shape[0]
    n_tok, model = acc.shape
    tok = n_tok // n
    ffn = w1.shape[2]
    half = 256
    acc[...] = jnp.zeros_like(acc)

    def body(e, _):
        gv = gb[e]
        for c in range(model // LANE):
            col = slice(c * LANE, (c + 1) * LANE)
            dy[:, col] = (gv * gg[:, :, col].reshape(n_tok, LANE).astype(F32)).astype(BF16)
        keep = mb[e] > 0.0
        keep = jnp.concatenate([keep, keep], axis=1)
        for c in range(ffn // half):
            col = slice(c * half, (c + 1) * half)
            dh = dot_nt(dy[...], w2[e, col, :])
            da_o[e, :, col] = jnp.where(keep, dh * pf[e, :, col], 0.0).astype(BF16)
            db_o[e, :, col] = jnp.where(keep, dh * qf[e, :, col], 0.0).astype(BF16)
        for c in range(model // half):
            col = slice(c * half, (c + 1) * half)
            stage[e, :, col] = dot(hT[e], dy[:, col]).astype(BF16)
            dr = dot_nt(da_o[e], w1[e, col, :]) + dot_nt(db_o[e], w3[e, col, :])
            acc[:, col] += dr.astype(BF16).astype(F32)
        pltpu.make_async_copy(stage.at[e], gwd_h.at[e], sem.at[e]).start()
        return 0

    lax.fori_loop(0, n_local, body, 0, unroll=2)
    for k, o in enumerate((own, s1, s2, s3)):
        blk = lax.bitwise_xor(me, k)
        o[...] = acc[pl.ds(pl.multiple_of(blk * tok, tok), tok), :]
    for e in range(n_local):
        pltpu.make_async_copy(stage.at[e], gwd_h.at[e], sem.at[e]).wait()


def wgrad_kernel(xT, da, db, g1_h, g3_h, st1, st3, sem):
    n_local = da.shape[0]
    half = 256

    def copies(e):
        return (pltpu.make_async_copy(st1.at[e], g1_h.at[e], sem.at[0, e]),
                pltpu.make_async_copy(st3.at[e], g3_h.at[e], sem.at[1, e]))

    def body(e, _):
        for c in range(da.shape[2] // half):
            col = slice(c * half, (c + 1) * half)
            st1[e, :, col] = dot(xT[...], da[e, :, col]).astype(BF16)
            st3[e, :, col] = dot(xT[...], db[e, :, col]).astype(BF16)
        for c in copies(e):
            c.start()
        return 0

    lax.fori_loop(0, n_local, body, 0, unroll=2)
    for e in range(n_local):
        for c in copies(e):
            c.wait()


def final_kernel(idx, slot, o0, o1, o2, o3, d0, d1, d2, d3, out, gx, ggate):
    model = out.shape[1]
    out[...] = (o0[:, :model] + o1[:, :model] + o2[:, :model] + o3[:, :model]).astype(BF16)
    gx[...] = (d0[...] + d1[...] + d2[...] + d3[...]).astype(BF16)
    dense = (o0[:, model:] + o1[:, model:] + o2[:, model:] + o3[:, model:]).T
    expert = lax.broadcasted_iota(jnp.int32, dense.shape, 0)
    for j in range(idx.shape[0]):
        hit = (expert == idx[j:j + 1, :]) & (slot[j:j + 1, :] >= 0)
        ggate[j:j + 1, :] = jnp.sum(jnp.where(hit, dense, 0.0), axis=0, keepdims=True)


def vm(shape, dtype):
    return pltpu.VMEM(shape, dtype)


def in_vmem(x):
    return pltpu.with_memory_space_constraint(x, pltpu.VMEM)


def in_hbm(x):
    return pltpu.with_memory_space_constraint(x, pltpu.HBM)


def solution(mesh):
    n = mesh.shape["ep"]
    row_spec = P(("dp", "ep"))
    expert_spec = P("ep")
    ANY = pl.BlockSpec(memory_space=pl.ANY)
    HB = pl.BlockSpec(memory_space=pltpu.HBM)
    VM = pl.BlockSpec(memory_space=pltpu.VMEM)

    def per_device(x_rows, expert_idx, gate_w, slot_pos, w_gate, w_up, w_down, grad_out):
        tok, model = x_rows.shape
        top = expert_idx.shape[1]
        nl, _, ffn = w_gate.shape
        nt = n * tok
        S = jax.ShapeDtypeStruct
        part = S((tok, model + LANE), F32)
        dpart = S((tok, model), F32)
        flops = 2 * nt * model * ffn * nl
        (w1, w3, w2, gg, gb, mb, hT, pf, qf, xT, *outs) = pl.pallas_call(
            functools.partial(forward_kernel, n),
            out_shape=(vm(w_gate.shape, BF16), vm(w_up.shape, BF16), vm(w_down.shape, BF16),
                       vm((n, tok, model), BF16),
                       vm((nl, nt, LANE), F32), vm((nl, nt, LANE), F32),
                       vm((nl, ffn, nt), BF16), vm((nl, nt, ffn), F32), vm((nl, nt, ffn), F32),
                       vm((model, nt), BF16), part, part, part, part),
            in_specs=[HB] * 8,
            out_specs=[VM] * 14,
            scratch_shapes=[
                pltpu.VMEM((n, tok, model), BF16),
                pltpu.VMEM((n, top, tok), jnp.int32), pltpu.VMEM((n, top, tok), F32), pltpu.VMEM((n, top, tok), jnp.int32),
                pltpu.VMEM((nl, nt, ffn), BF16), pltpu.VMEM((nt, model + LANE), F32),
                pltpu.SemaphoreType.DMA((5,)), pltpu.SemaphoreType.DMA((3, nl)),
                pltpu.SemaphoreType.DMA((5, 3)), pltpu.SemaphoreType.DMA((5, 3)),
            ],
            compiler_params=pltpu.CompilerParams(collective_id=0, has_side_effects=True, vmem_limit_bytes=8 << 20),
            cost_estimate=pl.CostEstimate(flops=3 * flops, bytes_accessed=25 << 20, transcendentals=0),
            name="moe_forward",
        )(*[in_hbm(v) for v in (expert_idx.T, gate_w.T, slot_pos.T, x_rows, grad_out, w_gate, w_up, w_down)])

        def swap(a, k):
            return lax.ppermute(a, "ep", [(i, i ^ k) for i in range(n)])

        o_recv = [swap(outs[k], k) for k in range(1, n)]

        gwd, da, db, *dxs = pl.pallas_call(
            functools.partial(dgrad_kernel, n),
            out_shape=(S(w_down.shape, BF16), vm((nl, nt, ffn), BF16), vm((nl, nt, ffn), BF16), dpart, dpart, dpart, dpart),
            in_specs=[VM] * 9,
            out_specs=[ANY] + [VM] * 6,
            scratch_shapes=[pltpu.VMEM((nt, model), BF16), pltpu.VMEM((nt, model), F32),
                            pltpu.VMEM(w_down.shape, BF16), pltpu.SemaphoreType.DMA((nl,))],
            cost_estimate=pl.CostEstimate(flops=4 * flops, bytes_accessed=10 << 20, transcendentals=0),
            compiler_params=pltpu.CompilerParams(vmem_limit_bytes=14 << 20),
            name="moe_dgrad",
        )(*[in_vmem(v) for v in (w1, w3, w2, gg, gb, mb, hT, pf, qf)])
        d_recv = [swap(dxs[k], k) for k in range(1, n)]

        gw1, gw3 = pl.pallas_call(
            wgrad_kernel,
            out_shape=(S(w_gate.shape, BF16), S(w_up.shape, BF16)),
            in_specs=[VM] * 3,
            out_specs=[ANY] * 2,
            scratch_shapes=[pltpu.VMEM(w_gate.shape, BF16), pltpu.VMEM(w_up.shape, BF16), pltpu.SemaphoreType.DMA((2, nl))],
            cost_estimate=pl.CostEstimate(flops=2 * flops, bytes_accessed=17 << 20, transcendentals=0),
            compiler_params=pltpu.CompilerParams(vmem_limit_bytes=20 << 20),
            name="moe_wgrad",
        )(*[in_vmem(v) for v in (xT, da, db)])

        out, gx, ggate = pl.pallas_call(
            final_kernel,
            out_shape=(S((tok, model), BF16), S((tok, model), BF16), S((top, tok), F32)),
            in_specs=[VM] * 10,
            out_specs=[VM] * 3,
            compiler_params=pltpu.CompilerParams(vmem_limit_bytes=8 << 20),
            name="moe_final",
        )(expert_idx.T, slot_pos.T, outs[0], *o_recv, dxs[0], *d_recv)
        return out, gx, gw1, gw3, gwd, ggate.T

    return jax.shard_map(per_device, mesh=mesh,
                         in_specs=(row_spec, row_spec, row_spec, row_spec, expert_spec, expert_spec, expert_spec, row_spec),
                         out_specs=(row_spec, row_spec, row_spec, row_spec, row_spec, row_spec),
                         check_vma=False)
```

```python
import functools

import jax
import jax.numpy as jnp
from jax import lax
from jax.experimental import pallas as pl
from jax.experimental.pallas import tpu as pltpu
from jax.sharding import PartitionSpec as P

F32 = jnp.float32
BF16 = jnp.bfloat16
MESH = pl.DeviceIdType.MESH
LANE = 128
NT = (((1,), (1,)), ((), ()))


def dot(a, b):
    return jnp.dot(a, b, preferred_element_type=F32)


def dot_nt(a, b):
    return lax.dot_general(a, b, NT, preferred_element_type=F32)


def token_kernel(n, unroll, idx_h, gate_h, slot_h, x_h, g_h, w1_h, w3_h, w2_h,
                 hT, dy, da, db, xT, own, out_send,
                 w1, w3, w2, xg, gg, idx_v, gate_v, slot_v, gb, mb, pf, qf, h_v, acc, inbox,
                 load_sem, w_sem, send_sem, recv_sem, part_send, part_recv):
    me = lax.axis_index("ep")
    sib, opp = lax.bitwise_xor(me, 1), lax.bitwise_xor(me, 2)
    diag = lax.bitwise_xor(me, 3)
    n_local = w1.shape[0]
    tok, model = x_h.shape
    ffn = w1.shape[2]
    n_tok = n * tok
    wide = model + LANE

    barrier = pltpu.get_barrier_semaphore()
    for other in (sib, opp):
        pl.semaphore_signal(barrier, inc=1, device_id={"ep": other}, device_id_type=MESH)

    srcs = (idx_h, gate_h, slot_h, x_h, g_h)
    bufs = (idx_v, gate_v, slot_v, xg, gg)
    loads = [pltpu.make_async_copy(s, b.at[me], load_sem.at[i]) for i, (s, b) in enumerate(zip(srcs, bufs))]
    for c in loads:
        c.start()

    def w_copy(k, e):
        wh, wv = ((w1_h, w1), (w3_h, w3), (w2_h, w2))[k]
        return pltpu.make_async_copy(wh.at[e], wv.at[e], w_sem.at[k, e])

    def send(i, block, to, k):
        return pltpu.make_async_remote_copy(
            src_ref=bufs[i].at[block], dst_ref=bufs[i].at[block],
            send_sem=send_sem.at[i, k], recv_sem=recv_sem.at[i, k],
            device_id={"ep": to}, device_id_type=MESH)

    for c in loads:
        c.wait()
    pl.semaphore_wait(barrier, 2)
    to_opp = [send(i, me, opp, 0) for i in range(5)]
    to_sib = [send(i, me, sib, 1) for i in range(5)]
    relay = [send(i, opp, sib, 2) for i in range(5)]
    for i in range(5):
        to_opp[i].start()
        to_sib[i].start()
    for e in range(n_local):
        for k in range(3):
            w_copy(k, e).start()
    acc[...] = jnp.zeros_like(acc)
    for i in range(3):
        to_opp[i].wait_recv()
        relay[i].start()
    for i in range(3):
        to_sib[i].wait_recv()
        relay[i].wait_recv()

    def rows_of(buf):
        return jnp.concatenate([buf[b] for b in range(n)], axis=1).T

    lane = lax.broadcasted_iota(jnp.int32, (n_tok, LANE), 1)
    ib, gt, sl = rows_of(idx_v), rows_of(gate_v), rows_of(slot_v)
    gd = jnp.zeros((n_tok, LANE), F32)
    md = jnp.zeros((n_tok, LANE), F32)
    for j in range(ib.shape[1]):
        hit = (ib[:, j:j + 1] == lane + me * n_local) & (sl[:, j:j + 1] >= 0)
        gd = jnp.where(hit, gt[:, j:j + 1], gd)
        md = jnp.where(hit, 1.0, md)
    for e in range(n_local):
        gb[e] = jnp.broadcast_to(gd[:, e:e + 1], (n_tok, LANE))
        mb[e] = jnp.broadcast_to(md[:, e:e + 1], (n_tok, LANE))

    for i in (3, 4):
        to_opp[i].wait_recv()
        relay[i].start()
    for i in (3, 4):
        to_sib[i].wait_recv()
        relay[i].wait_recv()
    xT[...] = xg[...].reshape(n_tok, model).T

    half = 256

    def expert(e, slot):
        for k in range(3):
            w_copy(k, e).wait()
        gv = gb[e]
        keep = mb[e] > 0.0
        keep = jnp.concatenate([keep, keep], axis=1)
        for c in range(model // LANE):
            col = slice(c * LANE, (c + 1) * LANE)
            dy[e, :, col] = (gv * gg[:, :, col].reshape(n_tok, LANE).astype(F32)).astype(BF16)
        for c in range(ffn // half):
            col = slice(c * half, (c + 1) * half)
            xv = xg[...].reshape(n_tok, model)
            a = dot(xv, w1[e, :, col])
            b = dot(xv, w3[e, :, col])
            sg = jax.nn.sigmoid(a)
            ga = a * sg
            h = jnp.where(keep, ga * b, 0.0).astype(BF16)
            h_v[slot, :, col] = h
            hT[e, col, :] = h.T
            dh = dot_nt(dy[e], w2[e, col, :])
            da[e, :, col] = jnp.where(keep, dh * (b * (sg * (1.0 + a * (1.0 - sg)))), 0.0).astype(BF16)
            db[e, :, col] = jnp.where(keep, dh * ga, 0.0).astype(BF16)
        part = jnp.zeros((n_tok, LANE), F32)
        for c in range(model // half):
            y = dot(h_v[slot], w2[e, :, c * half:(c + 1) * half]).astype(BF16).astype(F32)
            for k in range(half // LANE):
                yk = y[:, k * LANE:(k + 1) * LANE]
                col = slice(c * half + k * LANE, c * half + (k + 1) * LANE)
                acc[:, col] += gv * yk
                part += gg[:, :, col].reshape(n_tok, LANE).astype(F32) * yk
        row = jnp.sum(part, axis=1, keepdims=True)
        acc[:, model:wide] += jnp.where(lane == me * n_local + e, row, 0.0)
        for c in range(model // half):
            dr = dot_nt(da[e], w1[e, c * half:(c + 1) * half, :]) + dot_nt(db[e], w3[e, c * half:(c + 1) * half, :])
            acc[:, wide + c * half:wide + (c + 1) * half] += dr.astype(BF16).astype(F32)

    @pl.loop(0, n_local // unroll)
    def _(i):
        for u in range(unroll):
            expert(i * unroll + u, u)

    def rows(block):
        return pl.ds(pl.multiple_of(block * tok, tok), tok)

    swaps = [pltpu.make_async_remote_copy(
        src_ref=acc.at[rows(block)], dst_ref=inbox.at[k], send_sem=part_send.at[k], recv_sem=part_recv.at[k],
        device_id={"ep": sib}, device_id_type=MESH) for k, block in enumerate((diag, sib))]
    for c in swaps:
        c.start()
    swaps[0].wait_recv()
    out_send[...] = acc[rows(opp), :] + inbox[0]
    swaps[1].wait_recv()
    own[...] = acc[rows(me), :] + inbox[1]
    for c in swaps:
        c.wait_send()
    for i in range(5):
        to_opp[i].wait_send()
        to_sib[i].wait_send()
        relay[i].wait_send()


def wgrad_kernel(xT, hT, dy, da, db, g1_h, g3_h, g2_h, st1, st3, st2, sem):
    n_local = da.shape[0]
    half = 256

    def copy(k, e):
        st, gh = ((st2, g2_h), (st1, g1_h), (st3, g3_h))[k]
        return pltpu.make_async_copy(st.at[e], gh.at[e], sem.at[k, e])

    def body(e, _):
        for c in range(dy.shape[2] // half):
            col = slice(c * half, (c + 1) * half)
            st2[e, :, col] = dot(hT[e], dy[e, :, col]).astype(BF16)
        copy(0, e).start()
        for k, st, src in ((1, st1, da), (2, st3, db)):
            for c in range(da.shape[2] // half):
                col = slice(c * half, (c + 1) * half)
                st[e, :, col] = dot(xT[...], src[e, :, col]).astype(BF16)
            copy(k, e).start()
        return 0

    lax.fori_loop(0, n_local, body, 0, unroll=2)
    for e in range(n_local):
        for k in range(3):
            copy(k, e).wait()


def final_kernel(idx, slot, own, got, out, gx, ggate):
    model = out.shape[1]
    wide = model + LANE
    out[...] = (own[:, :model] + got[:, :model]).astype(BF16)
    gx[...] = (own[:, wide:] + got[:, wide:]).astype(BF16)
    dense = (own[:, model:wide] + got[:, model:wide]).T
    expert = lax.broadcasted_iota(jnp.int32, dense.shape, 0)
    for j in range(idx.shape[0]):
        hit = (expert == idx[j:j + 1, :]) & (slot[j:j + 1, :] >= 0)
        ggate[j:j + 1, :] = jnp.sum(jnp.where(hit, dense, 0.0), axis=0, keepdims=True)


def vm(shape, dtype):
    return pltpu.VMEM(shape, dtype)


def in_vmem(x):
    return pltpu.with_memory_space_constraint(x, pltpu.VMEM)


def in_hbm(x):
    return pltpu.with_memory_space_constraint(x, pltpu.HBM)


UNROLL = 2


def solution(mesh):
    n = mesh.shape["ep"]
    row_spec = P(("dp", "ep"))
    expert_spec = P("ep")
    ANY = pl.BlockSpec(memory_space=pl.ANY)
    HB = pl.BlockSpec(memory_space=pltpu.HBM)
    VM = pl.BlockSpec(memory_space=pltpu.VMEM)

    def per_device(x_rows, expert_idx, gate_w, slot_pos, w_gate, w_up, w_down, grad_out):
        tok, model = x_rows.shape
        top = expert_idx.shape[1]
        nl, _, ffn = w_gate.shape
        nt = n * tok
        S = jax.ShapeDtypeStruct
        width = 2 * model + LANE
        flops = 2 * nt * model * ffn * nl
        DMA = pltpu.SemaphoreType.DMA
        hT, dy, da, db, xT, own, opp_sum = pl.pallas_call(
            functools.partial(token_kernel, n, UNROLL),
            out_shape=(vm((nl, ffn, nt), BF16), vm((nl, nt, model), BF16), vm((nl, nt, ffn), BF16), vm((nl, nt, ffn), BF16),
                       vm((model, nt), BF16), vm((tok, width), F32), S((tok, width), F32)),
            in_specs=[HB] * 8,
            out_specs=[VM] * 7,
            scratch_shapes=[
                pltpu.VMEM(w_gate.shape, BF16), pltpu.VMEM(w_up.shape, BF16), pltpu.VMEM(w_down.shape, BF16),
                pltpu.VMEM((n, tok, model), BF16), pltpu.VMEM((n, tok, model), BF16),
                pltpu.VMEM((n, top, tok), jnp.int32), pltpu.VMEM((n, top, tok), F32), pltpu.VMEM((n, top, tok), jnp.int32),
                pltpu.VMEM((nl, nt, LANE), F32), pltpu.VMEM((nl, nt, LANE), F32),
                pltpu.VMEM((UNROLL, nt, ffn), F32), pltpu.VMEM((UNROLL, nt, ffn), F32), pltpu.VMEM((UNROLL, nt, ffn), BF16),
                pltpu.VMEM((nt, width), F32), pltpu.VMEM((2, tok, width), F32),
                DMA((5,)), DMA((3, nl)), DMA((5, 3)), DMA((5, 3)), DMA((2,)), DMA((2,)),
            ],
            compiler_params=pltpu.CompilerParams(collective_id=0, has_side_effects=True, vmem_limit_bytes=44 << 20),
            cost_estimate=pl.CostEstimate(flops=6 * flops, bytes_accessed=25 << 20, transcendentals=0),
            name="moe_tokens",
        )(*[in_hbm(v) for v in (expert_idx.T, gate_w.T, slot_pos.T, x_rows, grad_out, w_gate, w_up, w_down)])

        got = lax.ppermute(opp_sum, "ep", [(i, i ^ 2) for i in range(n)])

        gw1, gw3, gwd = pl.pallas_call(
            wgrad_kernel,
            out_shape=(S(w_gate.shape, BF16), S(w_up.shape, BF16), S(w_down.shape, BF16)),
            in_specs=[VM] * 5,
            out_specs=[ANY] * 3,
            scratch_shapes=[pltpu.VMEM(w_gate.shape, BF16), pltpu.VMEM(w_up.shape, BF16), pltpu.VMEM(w_down.shape, BF16),
                            DMA((3, nl))],
            compiler_params=pltpu.CompilerParams(vmem_limit_bytes=40 << 20),
            cost_estimate=pl.CostEstimate(flops=3 * flops, bytes_accessed=25 << 20, transcendentals=0),
            name="moe_wgrad",
        )(*[in_vmem(v) for v in (xT, hT, dy, da, db)])

        out, gx, ggate = pl.pallas_call(
            final_kernel,
            out_shape=(S((tok, model), BF16), S((tok, model), BF16), S((top, tok), F32)),
            in_specs=[VM] * 4,
            out_specs=[VM] * 3,
            compiler_params=pltpu.CompilerParams(vmem_limit_bytes=8 << 20),
            name="moe_final",
        )(expert_idx.T, slot_pos.T, in_vmem(own), got)
        return out, gx, gw1, gw3, gwd, ggate.T

    return jax.shard_map(per_device, mesh=mesh,
                         in_specs=(row_spec, row_spec, row_spec, row_spec, expert_spec, expert_spec, expert_spec, row_spec),
                         out_specs=(row_spec, row_spec, row_spec, row_spec, row_spec, row_spec),
                         check_vma=False)
```

```python
import functools

import jax
import jax.numpy as jnp
from jax import lax
from jax.experimental import pallas as pl
from jax.experimental.pallas import tpu as pltpu
from jax.sharding import PartitionSpec as P

F32 = jnp.float32
BF16 = jnp.bfloat16
MESH = pl.DeviceIdType.MESH
LANE = 128
NT = (((1,), (1,)), ((), ()))


def dot(a, b):
    return jnp.dot(a, b, preferred_element_type=F32)


def dot_nt(a, b):
    return lax.dot_general(a, b, NT, preferred_element_type=F32)


def token_kernel(n, unroll, idx_h, gate_h, slot_h, x_h, g_h, w1_h, w3_h, w2_h,
                 hT, dy, da, db, xT, own, out_send,
                 w1, w3, w2, w2T, w1T, xg, gg, idx_v, gate_v, slot_v, gb, mb, pf, qf, h_v, acc, inbox,
                 load_sem, w_sem, send_sem, recv_sem, part_send, part_recv):
    me = lax.axis_index("ep")
    sib, opp = lax.bitwise_xor(me, 1), lax.bitwise_xor(me, 2)
    diag = lax.bitwise_xor(me, 3)
    n_local = w1.shape[0]
    tok, model = x_h.shape
    ffn = w1.shape[2]
    n_tok = n * tok
    wide = model + LANE

    barrier = pltpu.get_barrier_semaphore()
    for other in (sib, opp, diag):
        pl.semaphore_signal(barrier, inc=1, device_id={"ep": other}, device_id_type=MESH)

    srcs = (idx_h, gate_h, slot_h, x_h, g_h)
    bufs = (idx_v, gate_v, slot_v, xg, gg)
    loads = [pltpu.make_async_copy(s, b.at[me], load_sem.at[i]) for i, (s, b) in enumerate(zip(srcs, bufs))]
    for c in loads:
        c.start()

    def w_copy(k, e):
        wh, wv = ((w1_h, w1), (w3_h, w3), (w2_h, w2))[k]
        return pltpu.make_async_copy(wh.at[e], wv.at[e], w_sem.at[k, e])

    def send(i, block, to, k):
        return pltpu.make_async_remote_copy(
            src_ref=bufs[i].at[block], dst_ref=bufs[i].at[block],
            send_sem=send_sem.at[i, k], recv_sem=recv_sem.at[i, k],
            device_id={"ep": to}, device_id_type=MESH)

    for c in loads:
        c.wait()
    pl.semaphore_wait(barrier, 3)
    to_opp = [send(i, me, opp, 0) for i in range(5)]
    to_sib = [send(i, me, sib, 1) for i in range(5)]
    relay = [send(i, opp, sib, 2) for i in range(4)] + [send(4, me, diag, 2)]
    for i in range(5):
        to_opp[i].start()
        to_sib[i].start()
    relay[4].start()
    for e in range(n_local):
        for k in range(3):
            w_copy(k, e).start()
    acc[...] = jnp.zeros_like(acc)
    for i in range(3):
        to_opp[i].wait_recv()
        relay[i].start()
    for i in range(3):
        to_sib[i].wait_recv()
        relay[i].wait_recv()

    def rows_of(buf):
        return jnp.concatenate([buf[b] for b in range(n)], axis=1).T

    lane = lax.broadcasted_iota(jnp.int32, (n_tok, LANE), 1)
    ib, gt, sl = rows_of(idx_v), rows_of(gate_v), rows_of(slot_v)
    gd = jnp.zeros((n_tok, LANE), F32)
    md = jnp.zeros((n_tok, LANE), F32)
    for j in range(ib.shape[1]):
        hit = (ib[:, j:j + 1] == lane + me * n_local) & (sl[:, j:j + 1] >= 0)
        gd = jnp.where(hit, gt[:, j:j + 1], gd)
        md = jnp.where(hit, 1.0, md)
    for e in range(n_local):
        gb[e] = jnp.broadcast_to(gd[:, e:e + 1], (n_tok, LANE))
        mb[e] = jnp.broadcast_to(md[:, e:e + 1], (n_tok, LANE))


    half = 256

    def ready(e):
        for k in range(3):
            w_copy(k, e).wait()

    def flip(e):
        if FLIP2:
            w2T[e % 2] = w2[e].T
        if FLIP1:
            w1T[e % 2] = w1[e].T

    def keep_of(e):
        keep = mb[e] > 0.0
        return jnp.concatenate([keep, keep], axis=1)

    def up(e, c):
        col = slice(c * half, (c + 1) * half)
        xv = xg[...].reshape(n_tok, model)
        a = dot(xv, w1[e, :, col])
        b = dot(xv, w3[e, :, col])
        sg = jax.nn.sigmoid(a)
        ga = a * sg
        h = jnp.where(keep_of(e), ga * b, 0.0).astype(BF16)
        h_v[e % UNROLL, :, col] = h
        hT[e, col, :] = h.T
        return b * (sg * (1.0 + a * (1.0 - sg))), ga

    def expert(e):
        gv = gb[e]
        for c in range(model // LANE):
            col = slice(c * LANE, (c + 1) * LANE)
            dy[e, :, col] = (gv * gg[:, :, col].reshape(n_tok, LANE).astype(F32)).astype(BF16)
        keep = keep_of(e)
        for c in range(ffn // half):
            col = slice(c * half, (c + 1) * half)
            pre, ga = (pf[e, :, col], qf[e, :, col]) if e < EARLY else up(e, c)
            dh = dot(dy[e], w2T[e % 2, :, col]) if FLIP2 else dot_nt(dy[e], w2[e, col, :])
            da[e, :, col] = jnp.where(keep, dh * pre, 0.0).astype(BF16)
            db[e, :, col] = jnp.where(keep, dh * ga, 0.0).astype(BF16)
        if e + 1 < n_local:
            flip(e + 1)
        part = jnp.zeros((n_tok, LANE), F32)
        for c in range(model // half):
            y = dot(h_v[e % UNROLL], w2[e, :, c * half:(c + 1) * half]).astype(BF16).astype(F32)
            for k in range(half // LANE):
                yk = y[:, k * LANE:(k + 1) * LANE]
                col = slice(c * half + k * LANE, c * half + (k + 1) * LANE)
                acc[:, col] += gv * yk
                part += gg[:, :, col].reshape(n_tok, LANE).astype(F32) * yk
        row = jnp.sum(part, axis=1, keepdims=True)
        acc[:, model:wide] += jnp.where(lane == me * n_local + e, row, 0.0)
        for c in range(model // half):
            col = slice(c * half, (c + 1) * half)
            dr = dot(da[e], w1T[e % 2, :, col]) if FLIP1 else dot_nt(da[e], w1[e, col, :])
            dr = dr + dot_nt(db[e], w3[e, col, :])
            acc[:, wide + c * half:wide + (c + 1) * half] += dr.astype(BF16).astype(F32)

    for e in range(EARLY):
        ready(e)
    to_opp[3].wait_recv()
    relay[3].start()
    flip(0)
    to_sib[3].wait_recv()
    relay[3].wait_recv()
    for e in range(EARLY):
        for c in range(ffn // half):
            col = slice(c * half, (c + 1) * half)
            pf[e, :, col], qf[e, :, col] = up(e, c)
    to_opp[4].wait_recv()
    xT[...] = xg[...].reshape(n_tok, model).T
    to_sib[4].wait_recv()
    relay[4].wait_recv()
    for e0 in range(0, n_local, unroll):
        for e in range(e0 + 1 if e0 else EARLY, min(e0 + unroll + 1, n_local)):
            ready(e)
        for e in range(e0, e0 + unroll):
            expert(e)

    def rows(block):
        return pl.ds(pl.multiple_of(block * tok, tok), tok)

    swaps = [pltpu.make_async_remote_copy(
        src_ref=acc.at[rows(block)], dst_ref=inbox.at[k], send_sem=part_send.at[k], recv_sem=part_recv.at[k],
        device_id={"ep": sib}, device_id_type=MESH) for k, block in enumerate((diag, sib))]
    for c in swaps:
        c.start()
    swaps[0].wait_recv()
    out_send[...] = acc[rows(opp), :] + inbox[0]
    swaps[1].wait_recv()
    own[...] = acc[rows(me), :] + inbox[1]
    for c in swaps:
        c.wait_send()
    for i in range(5):
        to_opp[i].wait_send()
        to_sib[i].wait_send()
        relay[i].wait_send()


def wgrad_kernel(xT, hT, dy, da, db, g1_h, g3_h, g2_h, st1, st3, st2, sem):
    n_local = da.shape[0]
    half = 256

    def copy(k, e):
        st, gh = ((st2, g2_h), (st1, g1_h), (st3, g3_h))[k]
        return pltpu.make_async_copy(st.at[e], gh.at[e], sem.at[k, e])

    def body(e, _):
        for c in range(dy.shape[2] // half):
            col = slice(c * half, (c + 1) * half)
            st2[e, :, col] = dot(hT[e], dy[e, :, col]).astype(BF16)
        copy(0, e).start()
        for k, st, src in ((1, st1, da), (2, st3, db)):
            for c in range(da.shape[2] // half):
                col = slice(c * half, (c + 1) * half)
                st[e, :, col] = dot(xT[...], src[e, :, col]).astype(BF16)
            copy(k, e).start()
        return 0

    lax.fori_loop(0, n_local, body, 0, unroll=2)
    for e in range(n_local):
        for k in range(3):
            copy(k, e).wait()


def final_kernel(idx, slot, own, got, out, gx, ggate):
    model = out.shape[1]
    wide = model + LANE
    out[...] = (own[:, :model] + got[:, :model]).astype(BF16)
    gx[...] = (own[:, wide:] + got[:, wide:]).astype(BF16)
    dense = (own[:, model:wide] + got[:, model:wide]).T
    expert = lax.broadcasted_iota(jnp.int32, dense.shape, 0)
    for j in range(idx.shape[0]):
        hit = (expert == idx[j:j + 1, :]) & (slot[j:j + 1, :] >= 0)
        ggate[j:j + 1, :] = jnp.sum(jnp.where(hit, dense, 0.0), axis=0, keepdims=True)


def vm(shape, dtype):
    return pltpu.VMEM(shape, dtype)


def in_vmem(x):
    return pltpu.with_memory_space_constraint(x, pltpu.VMEM)


def in_hbm(x):
    return pltpu.with_memory_space_constraint(x, pltpu.HBM)


UNROLL = 4
EARLY = 4
FLIP2 = True
FLIP1 = True


def solution(mesh):
    n = mesh.shape["ep"]
    row_spec = P(("dp", "ep"))
    expert_spec = P("ep")
    ANY = pl.BlockSpec(memory_space=pl.ANY)
    HB = pl.BlockSpec(memory_space=pltpu.HBM)
    VM = pl.BlockSpec(memory_space=pltpu.VMEM)

    def per_device(x_rows, expert_idx, gate_w, slot_pos, w_gate, w_up, w_down, grad_out):
        tok, model = x_rows.shape
        top = expert_idx.shape[1]
        nl, _, ffn = w_gate.shape
        nt = n * tok
        S = jax.ShapeDtypeStruct
        width = 2 * model + LANE
        flops = 2 * nt * model * ffn * nl
        DMA = pltpu.SemaphoreType.DMA
        hT, dy, da, db, xT, own, opp_sum = pl.pallas_call(
            functools.partial(token_kernel, n, UNROLL),
            out_shape=(vm((nl, ffn, nt), BF16), vm((nl, nt, model), BF16), vm((nl, nt, ffn), BF16), vm((nl, nt, ffn), BF16),
                       vm((model, nt), BF16), vm((tok, width), F32), S((tok, width), F32)),
            in_specs=[HB] * 8,
            out_specs=[VM] * 7,
            scratch_shapes=[
                pltpu.VMEM(w_gate.shape, BF16), pltpu.VMEM(w_up.shape, BF16), pltpu.VMEM(w_down.shape, BF16),
                pltpu.VMEM((2, model, ffn), BF16), pltpu.VMEM((2, ffn, model), BF16),
                pltpu.VMEM((n, tok, model), BF16), pltpu.VMEM((n, tok, model), BF16),
                pltpu.VMEM((n, top, tok), jnp.int32), pltpu.VMEM((n, top, tok), F32), pltpu.VMEM((n, top, tok), jnp.int32),
                pltpu.VMEM((nl, nt, LANE), F32), pltpu.VMEM((nl, nt, LANE), F32),
                pltpu.VMEM((EARLY, nt, ffn), F32), pltpu.VMEM((EARLY, nt, ffn), F32), pltpu.VMEM((UNROLL, nt, ffn), BF16),
                pltpu.VMEM((nt, width), F32), pltpu.VMEM((2, tok, width), F32),
                DMA((5,)), DMA((3, nl)), DMA((5, 3)), DMA((5, 3)), DMA((2,)), DMA((2,)),
            ],
            compiler_params=pltpu.CompilerParams(collective_id=0, has_side_effects=True, vmem_limit_bytes=44 << 20),
            cost_estimate=pl.CostEstimate(flops=6 * flops, bytes_accessed=25 << 20, transcendentals=0),
            name="moe_tokens",
        )(*[in_hbm(v) for v in (expert_idx.T, gate_w.T, slot_pos.T, x_rows, grad_out, w_gate, w_up, w_down)])

        got = lax.ppermute(opp_sum, "ep", [(i, i ^ 2) for i in range(n)])

        gw1, gw3, gwd = pl.pallas_call(
            wgrad_kernel,
            out_shape=(S(w_gate.shape, BF16), S(w_up.shape, BF16), S(w_down.shape, BF16)),
            in_specs=[VM] * 5,
            out_specs=[ANY] * 3,
            scratch_shapes=[pltpu.VMEM(w_gate.shape, BF16), pltpu.VMEM(w_up.shape, BF16), pltpu.VMEM(w_down.shape, BF16),
                            DMA((3, nl))],
            compiler_params=pltpu.CompilerParams(vmem_limit_bytes=40 << 20),
            cost_estimate=pl.CostEstimate(flops=3 * flops, bytes_accessed=25 << 20, transcendentals=0),
            name="moe_wgrad",
        )(*[in_vmem(v) for v in (xT, hT, dy, da, db)])

        out, gx, ggate = pl.pallas_call(
            final_kernel,
            out_shape=(S((tok, model), BF16), S((tok, model), BF16), S((top, tok), F32)),
            in_specs=[VM] * 4,
            out_specs=[VM] * 3,
            compiler_params=pltpu.CompilerParams(vmem_limit_bytes=8 << 20),
            name="moe_final",
        )(expert_idx.T, slot_pos.T, in_vmem(own), got)
        return out, gx, gw1, gw3, gwd, ggate.T

    return jax.shard_map(per_device, mesh=mesh,
                         in_specs=(row_spec, row_spec, row_spec, row_spec, expert_spec, expert_spec, expert_spec, row_spec),
                         out_specs=(row_spec, row_spec, row_spec, row_spec, row_spec, row_spec),
                         check_vma=False)
```

```python
import functools

import jax
import jax.numpy as jnp
from jax import lax
from jax.experimental import pallas as pl
from jax.experimental.pallas import tpu as pltpu
from jax.sharding import PartitionSpec as P

F32 = jnp.float32
BF16 = jnp.bfloat16
MESH = pl.DeviceIdType.MESH
LANE = 128
NT = (((1,), (1,)), ((), ()))


def dot(a, b):
    return jnp.dot(a, b, preferred_element_type=F32)


def dot_nt(a, b):
    return lax.dot_general(a, b, NT, preferred_element_type=F32)


def token_kernel(n, unroll, idx_h, gate_h, slot_h, x_h, g_h, w1_h, w3_h, w2_h,
                 hT, dy, da, db, xT, own, out_send,
                 w1, w3, w2, w2T, w1T, w3T, xg, gg, idx_v, gate_v, slot_v, gb, mb, pf, qf, h_v, acc, inbox,
                 load_sem, w_sem, send_sem, recv_sem, part_send, part_recv):
    me = lax.axis_index("ep")
    sib, opp = lax.bitwise_xor(me, 1), lax.bitwise_xor(me, 2)
    diag = lax.bitwise_xor(me, 3)
    n_local = w1.shape[0]
    tok, model = x_h.shape
    ffn = w1.shape[2]
    n_tok = n * tok
    wide = model + LANE

    barrier = pltpu.get_barrier_semaphore()
    for other in (sib, opp, diag):
        pl.semaphore_signal(barrier, inc=1, device_id={"ep": other}, device_id_type=MESH)

    srcs = (idx_h, gate_h, slot_h, x_h, g_h)
    bufs = (idx_v, gate_v, slot_v, xg, gg)
    loads = [pltpu.make_async_copy(s, b.at[me], load_sem.at[i]) for i, (s, b) in enumerate(zip(srcs, bufs))]
    for c in loads:
        c.start()

    def w_copy(k, e):
        wh, wv = ((w1_h, w1), (w3_h, w3), (w2_h, w2))[k]
        return pltpu.make_async_copy(wh.at[e], wv.at[e], w_sem.at[k, e])

    def send(i, block, to, k):
        return pltpu.make_async_remote_copy(
            src_ref=bufs[i].at[block], dst_ref=bufs[i].at[block],
            send_sem=send_sem.at[i, k], recv_sem=recv_sem.at[i, k],
            device_id={"ep": to}, device_id_type=MESH)

    for e in range(n_local):
        for k in range(3):
            w_copy(k, e).start(priority=1)
    for c in loads:
        c.wait()
    pl.semaphore_wait(barrier, 3)
    to_opp = [send(i, me, opp, 0) for i in range(5)]
    to_sib = [send(i, me, sib, 1) for i in range(5)]
    relay = [send(i, opp, sib, 2) for i in range(4)] + [send(4, me, diag, 2)]
    for i in range(5):
        to_opp[i].start()
        to_sib[i].start()
    relay[4].start()
    acc[...] = jnp.zeros_like(acc)
    def ready(e):
        for k in range(3):
            w_copy(k, e).wait()

    def flip(e):
        if FLIP2:
            w2T[e % TURNS] = w2[e].T
        if FLIP1:
            w1T[e % TURNS] = w1[e].T
        if FLIP3:
            w3T[e % TURNS] = w3[e].T

    def flips(lo, hi):
        for e in range(lo, hi):
            ready(e)
            flip(e)

    flips(0, CUTS[0])
    for i in range(3):
        to_opp[i].wait_recv()
        relay[i].start()
    flips(CUTS[0], CUTS[1])
    to_opp[3].wait_recv()
    relay[3].start()
    for i in range(3):
        to_sib[i].wait_recv()
        relay[i].wait_recv()

    def rows_of(buf):
        return jnp.concatenate([buf[b] for b in range(n)], axis=1).T

    lane = lax.broadcasted_iota(jnp.int32, (n_tok, LANE), 1)
    ib, gt, sl = rows_of(idx_v), rows_of(gate_v), rows_of(slot_v)
    gd = jnp.zeros((n_tok, LANE), F32)
    md = jnp.zeros((n_tok, LANE), F32)
    for j in range(ib.shape[1]):
        hit = (ib[:, j:j + 1] == lane + me * n_local) & (sl[:, j:j + 1] >= 0)
        gd = jnp.where(hit, gt[:, j:j + 1], gd)
        md = jnp.where(hit, 1.0, md)
    for e in range(n_local):
        gb[e] = jnp.broadcast_to(gd[:, e:e + 1], (n_tok, LANE))
        mb[e] = jnp.broadcast_to(md[:, e:e + 1], (n_tok, LANE))


    half = 256

    def rows(block):
        return pl.ds(pl.multiple_of(block * tok, tok), tok)

    spans = (pl.ds(0, wide), pl.ds(wide, model))

    def swap(k, b):
        block = (diag, sib)[b]
        return pltpu.make_async_remote_copy(
            src_ref=acc.at[rows(block), spans[k]], dst_ref=inbox.at[b, :, spans[k]],
            send_sem=part_send.at[k, b], recv_sem=part_recv.at[k, b],
            device_id={"ep": sib}, device_id_type=MESH)

    def start_swap(k):
        for b in range(2):
            swap(k, b).start()

    def keep_of(e):
        keep = mb[e] > 0.0
        return jnp.concatenate([keep, keep], axis=1)

    def up(e, c):
        col = slice(c * half, (c + 1) * half)
        xv = xg[...].reshape(n_tok, model)
        a = dot(xv, w1[e, :, col])
        b = dot(xv, w3[e, :, col])
        sg = jax.nn.sigmoid(a)
        ga = a * sg
        h = jnp.where(keep_of(e), ga * b, 0.0).astype(BF16)
        h_v[e % UNROLL, :, col] = h
        hT[e, col, :] = h.T
        return b * (sg * (1.0 + a * (1.0 - sg))), ga

    def expert(e):
        gv = gb[e]
        for c in range(model // LANE):
            col = slice(c * LANE, (c + 1) * LANE)
            dy[e, :, col] = (gv * gg[:, :, col].reshape(n_tok, LANE).astype(F32)).astype(BF16)
        keep = keep_of(e)
        for c in range(ffn // half):
            col = slice(c * half, (c + 1) * half)
            pre, ga = (pf[e, :, col], qf[e, :, col]) if e < EARLY else up(e, c)
            dh = dot(dy[e], w2T[e % TURNS, :, col]) if FLIP2 else dot_nt(dy[e], w2[e, col, :])
            da[e, :, col] = jnp.where(keep, dh * pre, 0.0).astype(BF16)
            db[e, :, col] = jnp.where(keep, dh * ga, 0.0).astype(BF16)
        if e + CUTS[2] < n_local:
            flip(e + CUTS[2])
        part = jnp.zeros((n_tok, LANE), F32)
        for c in range(model // half):
            y = dot(h_v[e % UNROLL], w2[e, :, c * half:(c + 1) * half]).astype(BF16).astype(F32)
            for k in range(half // LANE):
                yk = y[:, k * LANE:(k + 1) * LANE]
                col = slice(c * half + k * LANE, c * half + (k + 1) * LANE)
                acc[:, col] += gv * yk
                part += gg[:, :, col].reshape(n_tok, LANE).astype(F32) * yk
        row = jnp.sum(part, axis=1, keepdims=True)
        acc[:, model:wide] += jnp.where(lane == me * n_local + e, row, 0.0)
        if e + 1 == n_local:
            start_swap(0)
        for c in range(model // half):
            col = slice(c * half, (c + 1) * half)
            both = jnp.concatenate([da[e], db[e]], axis=1)
            dr = dot(both, jnp.concatenate([w1T[e % TURNS, :, col], w3T[e % TURNS, :, col]], axis=0))
            acc[:, wide + c * half:wide + (c + 1) * half] += dr.astype(BF16).astype(F32)

    flips(CUTS[1], CUTS[2])
    for e in range(CUTS[2], EARLY):
        ready(e)
    to_sib[3].wait_recv()
    relay[3].wait_recv()
    for e in range(EARLY):
        for c in range(ffn // half):
            col = slice(c * half, (c + 1) * half)
            pf[e, :, col], qf[e, :, col] = up(e, c)
    to_opp[4].wait_recv()
    xT[...] = xg[...].reshape(n_tok, model).T
    to_sib[4].wait_recv()
    relay[4].wait_recv()
    for e0 in range(0, n_local, unroll):
        for e in range(max(EARLY, CUTS[2], e0 + CUTS[2] if e0 else 0), min(e0 + unroll + CUTS[2], n_local)):
            ready(e)
        for e in range(e0, e0 + unroll):
            expert(e)

    start_swap(1)
    for k, col in enumerate(spans):
        swap(k, 0).wait_recv()
        out_send[:, col] = acc[rows(opp), col] + inbox[0, :, col]
        swap(k, 1).wait_recv()
        own[:, col] = acc[rows(me), col] + inbox[1, :, col]
    for k in range(2):
        for b in range(2):
            swap(k, b).wait_send()
    for i in range(5):
        to_opp[i].wait_send()
        to_sib[i].wait_send()
        relay[i].wait_send()


def wgrad_kernel(xT, hT, dy, da, db, g1_h, g3_h, g2_h, st1, st3, st2, sem):
    n_local = da.shape[0]
    half = 256

    def copy(k, e):
        st, gh = ((st2, g2_h), (st1, g1_h), (st3, g3_h))[k]
        return pltpu.make_async_copy(st.at[e], gh.at[e], sem.at[k, e])

    def body(e, _):
        for c in range(dy.shape[2] // half):
            col = slice(c * half, (c + 1) * half)
            st2[e, :, col] = dot(hT[e], dy[e, :, col]).astype(BF16)
        copy(0, e).start()
        for k, st, src in ((1, st1, da), (2, st3, db)):
            for c in range(da.shape[2] // half):
                col = slice(c * half, (c + 1) * half)
                st[e, :, col] = dot(xT[...], src[e, :, col]).astype(BF16)
            copy(k, e).start()
        return 0

    lax.fori_loop(0, n_local, body, 0, unroll=2)
    for e in range(n_local):
        for k in range(3):
            copy(k, e).wait()


def final_kernel(idx, slot, own, got, out, gx, ggate):
    model = out.shape[1]
    wide = model + LANE
    out[...] = (own[:, :model] + got[:, :model]).astype(BF16)
    gx[...] = (own[:, wide:] + got[:, wide:]).astype(BF16)
    dense = (own[:, model:wide] + got[:, model:wide]).T
    expert = lax.broadcasted_iota(jnp.int32, dense.shape, 0)
    for j in range(idx.shape[0]):
        hit = (expert == idx[j:j + 1, :]) & (slot[j:j + 1, :] >= 0)
        ggate[j:j + 1, :] = jnp.sum(jnp.where(hit, dense, 0.0), axis=0, keepdims=True)


def vm(shape, dtype):
    return pltpu.VMEM(shape, dtype)


def in_vmem(x):
    return pltpu.with_memory_space_constraint(x, pltpu.VMEM)


def in_hbm(x):
    return pltpu.with_memory_space_constraint(x, pltpu.HBM)


UNROLL = 4
EARLY = 4
CUTS = (2, 4, 4)
TURNS = 5
FLIP2 = True
FLIP1 = True
FLIP3 = True


def solution(mesh):
    n = mesh.shape["ep"]
    row_spec = P(("dp", "ep"))
    expert_spec = P("ep")
    ANY = pl.BlockSpec(memory_space=pl.ANY)
    HB = pl.BlockSpec(memory_space=pltpu.HBM)
    VM = pl.BlockSpec(memory_space=pltpu.VMEM)

    def per_device(x_rows, expert_idx, gate_w, slot_pos, w_gate, w_up, w_down, grad_out):
        tok, model = x_rows.shape
        top = expert_idx.shape[1]
        nl, _, ffn = w_gate.shape
        nt = n * tok
        S = jax.ShapeDtypeStruct
        width = 2 * model + LANE
        flops = 2 * nt * model * ffn * nl
        DMA = pltpu.SemaphoreType.DMA
        hT, dy, da, db, xT, own, opp_sum = pl.pallas_call(
            functools.partial(token_kernel, n, UNROLL),
            out_shape=(vm((nl, ffn, nt), BF16), vm((nl, nt, model), BF16), vm((nl, nt, ffn), BF16), vm((nl, nt, ffn), BF16),
                       vm((model, nt), BF16), vm((tok, width), F32), S((tok, width), F32)),
            in_specs=[HB] * 8,
            out_specs=[VM] * 7,
            scratch_shapes=[
                pltpu.VMEM(w_gate.shape, BF16), pltpu.VMEM(w_up.shape, BF16), pltpu.VMEM(w_down.shape, BF16),
                pltpu.VMEM((TURNS, model, ffn), BF16), pltpu.VMEM((TURNS, ffn, model), BF16), pltpu.VMEM((TURNS, ffn, model), BF16),
                pltpu.VMEM((n, tok, model), BF16), pltpu.VMEM((n, tok, model), BF16),
                pltpu.VMEM((n, top, tok), jnp.int32), pltpu.VMEM((n, top, tok), F32), pltpu.VMEM((n, top, tok), jnp.int32),
                pltpu.VMEM((nl, nt, LANE), F32), pltpu.VMEM((nl, nt, LANE), F32),
                pltpu.VMEM((EARLY, nt, ffn), F32), pltpu.VMEM((EARLY, nt, ffn), F32), pltpu.VMEM((UNROLL, nt, ffn), BF16),
                pltpu.VMEM((nt, width), F32), pltpu.VMEM((2, tok, width), F32),
                DMA((5,)), DMA((3, nl)), DMA((5, 3)), DMA((5, 3)), DMA((2, 2)), DMA((2, 2)),
            ],
            compiler_params=pltpu.CompilerParams(collective_id=0, has_side_effects=True, vmem_limit_bytes=52 << 20),
            cost_estimate=pl.CostEstimate(flops=6 * flops, bytes_accessed=25 << 20, transcendentals=0),
            name="moe_tokens",
        )(*[in_hbm(v) for v in (expert_idx.T, gate_w.T, slot_pos.T, x_rows, grad_out, w_gate, w_up, w_down)])

        got = lax.ppermute(opp_sum, "ep", [(i, i ^ 2) for i in range(n)])

        gw1, gw3, gwd = pl.pallas_call(
            wgrad_kernel,
            out_shape=(S(w_gate.shape, BF16), S(w_up.shape, BF16), S(w_down.shape, BF16)),
            in_specs=[VM] * 5,
            out_specs=[ANY] * 3,
            scratch_shapes=[pltpu.VMEM(w_gate.shape, BF16), pltpu.VMEM(w_up.shape, BF16), pltpu.VMEM(w_down.shape, BF16),
                            DMA((3, nl))],
            compiler_params=pltpu.CompilerParams(vmem_limit_bytes=40 << 20),
            cost_estimate=pl.CostEstimate(flops=3 * flops, bytes_accessed=25 << 20, transcendentals=0),
            name="moe_wgrad",
        )(*[in_vmem(v) for v in (xT, hT, dy, da, db)])

        out, gx, ggate = pl.pallas_call(
            final_kernel,
            out_shape=(S((tok, model), BF16), S((tok, model), BF16), S((top, tok), F32)),
            in_specs=[VM] * 4,
            out_specs=[VM] * 3,
            compiler_params=pltpu.CompilerParams(vmem_limit_bytes=8 << 20),
            name="moe_final",
        )(expert_idx.T, slot_pos.T, in_vmem(own), got)
        return out, gx, gw1, gw3, gwd, ggate.T

    return jax.shard_map(per_device, mesh=mesh,
                         in_specs=(row_spec, row_spec, row_spec, row_spec, expert_spec, expert_spec, expert_spec, row_spec),
                         out_specs=(row_spec, row_spec, row_spec, row_spec, row_spec, row_spec),
                         check_vma=False)
```

```python
import functools

import jax
import jax.numpy as jnp
from jax import lax
from jax.experimental import pallas as pl
from jax.experimental.pallas import tpu as pltpu
from jax.sharding import PartitionSpec as P

F32 = jnp.float32
BF16 = jnp.bfloat16
MESH = pl.DeviceIdType.MESH
LANE = 128
NT = (((1,), (1,)), ((), ()))


def dot(a, b):
    return jnp.dot(a, b, preferred_element_type=F32)


def dot_nt(a, b):
    return lax.dot_general(a, b, NT, preferred_element_type=F32)


def token_kernel(n, unroll, idx_h, gate_h, slot_h, x_h, g_h, w1_h, w3_h, w2_h,
                 hT, dy, da, db, xT, own, out_send,
                 w1, w3, w2, w2T, w1T, w3T, xg, gg, idx_v, gate_v, slot_v, gb, mb, pf, qf, h_v, acc, inbox,
                 load_sem, w_sem, send_sem, recv_sem, part_send, part_recv):
    me = lax.axis_index("ep")
    sib, opp = lax.bitwise_xor(me, 1), lax.bitwise_xor(me, 2)
    diag = lax.bitwise_xor(me, 3)
    n_local = w1.shape[0]
    tok, model = x_h.shape
    ffn = w1.shape[2]
    n_tok = n * tok
    wide = model + LANE

    barrier = pltpu.get_barrier_semaphore()
    for other in (sib, opp, diag):
        pl.semaphore_signal(barrier, inc=1, device_id={"ep": other}, device_id_type=MESH)

    srcs = (idx_h, gate_h, slot_h, x_h, g_h)
    bufs = (idx_v, gate_v, slot_v, xg, gg)
    loads = [pltpu.make_async_copy(s, b.at[me], load_sem.at[i]) for i, (s, b) in enumerate(zip(srcs, bufs))]
    for c in loads:
        c.start()

    def w_copy(k, e):
        wh, wv = ((w1_h, w1), (w3_h, w3), (w2_h, w2))[k]
        return pltpu.make_async_copy(wh.at[e], wv.at[e], w_sem.at[k, e])

    def send(i, block, to, k):
        return pltpu.make_async_remote_copy(
            src_ref=bufs[i].at[block], dst_ref=bufs[i].at[block],
            send_sem=send_sem.at[i, k], recv_sem=recv_sem.at[i, k],
            device_id={"ep": to}, device_id_type=MESH)

    for e in range(n_local):
        for k in range(3):
            w_copy(k, e).start(priority=1)
    for c in loads:
        c.wait()
    pl.semaphore_wait(barrier, 3)
    to_opp = [send(i, me, opp, 0) for i in range(5)]
    to_sib = [send(i, me, sib, 1) for i in range(5)]
    relay = [send(i, opp, sib, 2) for i in range(4)] + [send(4, me, diag, 2)]
    for i in range(5):
        to_opp[i].start()
        to_sib[i].start()
    relay[4].start()
    acc[...] = jnp.zeros_like(acc)
    def ready(e):
        for k in range(3):
            w_copy(k, e).wait()

    def flip(e):
        if FLIP2:
            w2T[e % TURNS] = w2[e].T
        if FLIP1:
            w1T[e % TURNS] = w1[e].T
        if FLIP3:
            w3T[e % TURNS] = w3[e].T

    def flips(lo, hi):
        for e in range(lo, hi):
            ready(e)
            flip(e)

    flips(0, CUTS[0])
    for i in range(3):
        to_opp[i].wait_recv()
        relay[i].start()
    flips(CUTS[0], CUTS[1])
    to_opp[3].wait_recv()
    relay[3].start()
    for i in range(3):
        to_sib[i].wait_recv()
        relay[i].wait_recv()

    def rows_of(buf):
        return jnp.concatenate([buf[b] for b in range(n)], axis=1).T

    lane = lax.broadcasted_iota(jnp.int32, (n_tok, LANE), 1)
    ib, gt, sl = rows_of(idx_v), rows_of(gate_v), rows_of(slot_v)
    gd = jnp.zeros((n_tok, LANE), F32)
    md = jnp.zeros((n_tok, LANE), F32)
    for j in range(ib.shape[1]):
        hit = (ib[:, j:j + 1] == lane + me * n_local) & (sl[:, j:j + 1] >= 0)
        gd = jnp.where(hit, gt[:, j:j + 1], gd)
        md = jnp.where(hit, 1.0, md)
    for e in range(n_local):
        gb[e] = jnp.broadcast_to(gd[:, e:e + 1], (n_tok, LANE))
        mb[e] = jnp.broadcast_to(md[:, e:e + 1], (n_tok, LANE))


    half = 256

    def rows(block):
        return pl.ds(pl.multiple_of(block * tok, tok), tok)

    spans = (pl.ds(0, wide), pl.ds(wide, model))

    def swap(k, b):
        block = (diag, sib)[b]
        return pltpu.make_async_remote_copy(
            src_ref=acc.at[rows(block), spans[k]], dst_ref=inbox.at[b, :, spans[k]],
            send_sem=part_send.at[k, b], recv_sem=part_recv.at[k, b],
            device_id={"ep": sib}, device_id_type=MESH)

    def start_swap(k):
        for b in range(2):
            swap(k, b).start()

    def keep_of(e):
        keep = mb[e] > 0.0
        return jnp.concatenate([keep, keep], axis=1)

    def up(e, c):
        col = slice(c * half, (c + 1) * half)
        xv = xg[...].reshape(n_tok, model)
        keep = keep_of(e)
        a = jnp.where(keep, dot(xv, w1[e, :, col]), 0.0)
        b = jnp.where(keep, dot(xv, w3[e, :, col]), 0.0)
        sg = jax.nn.sigmoid(a)
        ga = a * sg
        h = (ga * b).astype(BF16)
        h_v[e, :, col] = h
        hT[e, col, :] = h.T
        return b * (sg * (1.0 + a * (1.0 - sg))), ga

    def expert(e):
        gv = gb[e]
        for c in range(model // LANE):
            col = slice(c * LANE, (c + 1) * LANE)
            dy[e, :, col] = (gv * gg[:, :, col].reshape(n_tok, LANE).astype(F32)).astype(BF16)
        for c in range(ffn // half):
            col = slice(c * half, (c + 1) * half)
            pre, ga = (pf[e, :, col], qf[e, :, col]) if e < EARLY else up(e, c)
            dh = dot(dy[e], w2T[e % TURNS, :, col]) if FLIP2 else dot_nt(dy[e], w2[e, col, :])
            da[e, :, col] = (dh * pre).astype(BF16)
            db[e, :, col] = (dh * ga).astype(BF16)
        if e + CUTS[2] < n_local:
            flip(e + CUTS[2])
        part = jnp.zeros((n_tok, LANE), F32)
        for c in range(model // half):
            y = dot(h_v[e], w2[e, :, c * half:(c + 1) * half]).astype(BF16).astype(F32)
            for k in range(half // LANE):
                yk = y[:, k * LANE:(k + 1) * LANE]
                col = slice(c * half + k * LANE, c * half + (k + 1) * LANE)
                acc[:, col] += gv * yk
                part += gg[:, :, col].reshape(n_tok, LANE).astype(F32) * yk
        row = jnp.sum(part, axis=1, keepdims=True)
        acc[:, model:wide] += jnp.where(lane == me * n_local + e, row, 0.0)
        if e + 1 == n_local:
            start_swap(0)
        for c in range(model // half):
            col = slice(c * half, (c + 1) * half)
            both = jnp.concatenate([da[e], db[e]], axis=1)
            dr = dot(both, jnp.concatenate([w1T[e % TURNS, :, col], w3T[e % TURNS, :, col]], axis=0))
            acc[:, wide + c * half:wide + (c + 1) * half] += dr.astype(BF16).astype(F32)

    flips(CUTS[1], CUTS[2])
    for e in range(CUTS[2], EARLY):
        ready(e)
    to_sib[3].wait_recv()
    relay[3].wait_recv()
    for e in range(EARLY):
        for c in range(ffn // half):
            col = slice(c * half, (c + 1) * half)
            pf[e, :, col], qf[e, :, col] = up(e, c)
    to_opp[4].wait_recv()
    xT[...] = xg[...].reshape(n_tok, model).T
    to_sib[4].wait_recv()
    relay[4].wait_recv()
    for e0 in range(0, n_local, unroll):
        for e in range(max(EARLY, CUTS[2], e0 + CUTS[2] if e0 else 0), min(e0 + unroll + CUTS[2], n_local)):
            ready(e)
        for e in range(e0, e0 + unroll):
            expert(e)

    start_swap(1)
    for k, col in enumerate(spans):
        swap(k, 0).wait_recv()
        out_send[:, col] = acc[rows(opp), col] + inbox[0, :, col]
        swap(k, 1).wait_recv()
        own[:, col] = acc[rows(me), col] + inbox[1, :, col]
    for k in range(2):
        for b in range(2):
            swap(k, b).wait_send()
    for i in range(5):
        to_opp[i].wait_send()
        to_sib[i].wait_send()
        relay[i].wait_send()


def wgrad_kernel(xT, hT, dy, da, db, g1_h, g3_h, g2_h, st1, st3, st2, sem):
    n_local = da.shape[0]
    half = 256

    def copy(k, e):
        st, gh = ((st2, g2_h), (st1, g1_h), (st3, g3_h))[k]
        return pltpu.make_async_copy(st.at[e], gh.at[e], sem.at[k, e])

    def body(e, _):
        for c in range(dy.shape[2] // half):
            col = slice(c * half, (c + 1) * half)
            st2[e, :, col] = dot(hT[e], dy[e, :, col]).astype(BF16)
        copy(0, e).start()
        for k, st, src in ((1, st1, da), (2, st3, db)):
            for c in range(da.shape[2] // half):
                col = slice(c * half, (c + 1) * half)
                st[e, :, col] = dot(xT[...], src[e, :, col]).astype(BF16)
            copy(k, e).start()
        return 0

    lax.fori_loop(0, n_local, body, 0, unroll=2)
    for e in range(n_local):
        for k in range(3):
            copy(k, e).wait()


def final_kernel(idx, slot, own, got, out, gx, ggate):
    model = out.shape[1]
    wide = model + LANE
    out[...] = (own[:, :model] + got[:, :model]).astype(BF16)
    gx[...] = (own[:, wide:] + got[:, wide:]).astype(BF16)
    dense = (own[:, model:wide] + got[:, model:wide]).T
    expert = lax.broadcasted_iota(jnp.int32, dense.shape, 0)
    for j in range(idx.shape[0]):
        hit = (expert == idx[j:j + 1, :]) & (slot[j:j + 1, :] >= 0)
        ggate[j:j + 1, :] = jnp.sum(jnp.where(hit, dense, 0.0), axis=0, keepdims=True)


def vm(shape, dtype):
    return pltpu.VMEM(shape, dtype)


def in_vmem(x):
    return pltpu.with_memory_space_constraint(x, pltpu.VMEM)


def in_hbm(x):
    return pltpu.with_memory_space_constraint(x, pltpu.HBM)


UNROLL = 4
EARLY = 6
CUTS = (2, 4, 4)
TURNS = 5
FLIP2 = True
FLIP1 = True
FLIP3 = True


def solution(mesh):
    n = mesh.shape["ep"]
    row_spec = P(("dp", "ep"))
    expert_spec = P("ep")
    ANY = pl.BlockSpec(memory_space=pl.ANY)
    HB = pl.BlockSpec(memory_space=pltpu.HBM)
    VM = pl.BlockSpec(memory_space=pltpu.VMEM)

    def per_device(x_rows, expert_idx, gate_w, slot_pos, w_gate, w_up, w_down, grad_out):
        tok, model = x_rows.shape
        top = expert_idx.shape[1]
        nl, _, ffn = w_gate.shape
        nt = n * tok
        S = jax.ShapeDtypeStruct
        width = 2 * model + LANE
        flops = 2 * nt * model * ffn * nl
        DMA = pltpu.SemaphoreType.DMA
        hT, dy, da, db, xT, own, opp_sum = pl.pallas_call(
            functools.partial(token_kernel, n, UNROLL),
            out_shape=(vm((nl, ffn, nt), BF16), vm((nl, nt, model), BF16), vm((nl, nt, ffn), BF16), vm((nl, nt, ffn), BF16),
                       vm((model, nt), BF16), vm((tok, width), F32), S((tok, width), F32)),
            in_specs=[HB] * 8,
            out_specs=[VM] * 7,
            scratch_shapes=[
                pltpu.VMEM(w_gate.shape, BF16), pltpu.VMEM(w_up.shape, BF16), pltpu.VMEM(w_down.shape, BF16),
                pltpu.VMEM((TURNS, model, ffn), BF16), pltpu.VMEM((TURNS, ffn, model), BF16), pltpu.VMEM((TURNS, ffn, model), BF16),
                pltpu.VMEM((n, tok, model), BF16), pltpu.VMEM((n, tok, model), BF16),
                pltpu.VMEM((n, top, tok), jnp.int32), pltpu.VMEM((n, top, tok), F32), pltpu.VMEM((n, top, tok), jnp.int32),
                pltpu.VMEM((nl, nt, LANE), F32), pltpu.VMEM((nl, nt, LANE), F32),
                pltpu.VMEM((EARLY, nt, ffn), F32), pltpu.VMEM((EARLY, nt, ffn), F32), pltpu.VMEM((nl, nt, ffn), BF16),
                pltpu.VMEM((nt, width), F32), pltpu.VMEM((2, tok, width), F32),
                DMA((5,)), DMA((3, nl)), DMA((5, 3)), DMA((5, 3)), DMA((2, 2)), DMA((2, 2)),
            ],
            compiler_params=pltpu.CompilerParams(collective_id=0, has_side_effects=True, vmem_limit_bytes=57 << 20),
            cost_estimate=pl.CostEstimate(flops=6 * flops, bytes_accessed=25 << 20, transcendentals=0),
            name="moe_tokens",
        )(*[in_hbm(v) for v in (expert_idx.T, gate_w.T, slot_pos.T, x_rows, grad_out, w_gate, w_up, w_down)])

        got = lax.ppermute(opp_sum, "ep", [(i, i ^ 2) for i in range(n)])

        gw1, gw3, gwd = pl.pallas_call(
            wgrad_kernel,
            out_shape=(S(w_gate.shape, BF16), S(w_up.shape, BF16), S(w_down.shape, BF16)),
            in_specs=[VM] * 5,
            out_specs=[ANY] * 3,
            scratch_shapes=[pltpu.VMEM(w_gate.shape, BF16), pltpu.VMEM(w_up.shape, BF16), pltpu.VMEM(w_down.shape, BF16),
                            DMA((3, nl))],
            compiler_params=pltpu.CompilerParams(vmem_limit_bytes=40 << 20),
            cost_estimate=pl.CostEstimate(flops=3 * flops, bytes_accessed=25 << 20, transcendentals=0),
            name="moe_wgrad",
        )(*[in_vmem(v) for v in (xT, hT, dy, da, db)])

        out, gx, ggate = pl.pallas_call(
            final_kernel,
            out_shape=(S((tok, model), BF16), S((tok, model), BF16), S((top, tok), F32)),
            in_specs=[VM] * 4,
            out_specs=[VM] * 3,
            compiler_params=pltpu.CompilerParams(vmem_limit_bytes=8 << 20),
            name="moe_final",
        )(expert_idx.T, slot_pos.T, in_vmem(own), got)
        return out, gx, gw1, gw3, gwd, ggate.T

    return jax.shard_map(per_device, mesh=mesh,
                         in_specs=(row_spec, row_spec, row_spec, row_spec, expert_spec, expert_spec, expert_spec, row_spec),
                         out_specs=(row_spec, row_spec, row_spec, row_spec, row_spec, row_spec),
                         check_vma=False)
```

```python
import functools

import jax
import jax.numpy as jnp
from jax import lax
from jax.experimental import pallas as pl
from jax.experimental.pallas import tpu as pltpu
from jax.sharding import PartitionSpec as P

F32 = jnp.float32
BF16 = jnp.bfloat16
MESH = pl.DeviceIdType.MESH
LANE = 128
NT = (((1,), (1,)), ((), ()))


def dot(a, b):
    return jnp.dot(a, b, preferred_element_type=F32)


def dot_nt(a, b):
    return lax.dot_general(a, b, NT, preferred_element_type=F32)


def token_kernel(n, unroll, idx_h, gate_h, slot_h, x_h, g_h, w1_h, w3_h, w2_h,
                 hT, dy, da, db, xT, own, out_send,
                 w1, w3, w2, w2T, w1T, w3T, xg, gg, idx_v, gate_v, slot_v, gb, mb, pf, qf, h_v, acc, inbox,
                 load_sem, w_sem, send_sem, recv_sem, part_send, part_recv):
    me = lax.axis_index("ep")
    sib, opp = lax.bitwise_xor(me, 1), lax.bitwise_xor(me, 2)
    diag = lax.bitwise_xor(me, 3)
    n_local = w1.shape[0]
    tok, model = x_h.shape
    ffn = w1.shape[2]
    n_tok = n * tok
    wide = model + LANE

    barrier = pltpu.get_barrier_semaphore()
    for other in (sib, opp, diag):
        pl.semaphore_signal(barrier, inc=1, device_id={"ep": other}, device_id_type=MESH)

    srcs = (idx_h, gate_h, slot_h, x_h, g_h)
    bufs = (idx_v, gate_v, slot_v, xg, gg)
    loads = [pltpu.make_async_copy(s, b.at[me], load_sem.at[i]) for i, (s, b) in enumerate(zip(srcs, bufs))]
    for c in loads:
        c.start()

    def w_copy(k, e):
        wh, wv = ((w1_h, w1), (w3_h, w3), (w2_h, w2))[k]
        return pltpu.make_async_copy(wh.at[e], wv.at[e], w_sem.at[k, e])

    def send(i, block, to, k):
        return pltpu.make_async_remote_copy(
            src_ref=bufs[i].at[block], dst_ref=bufs[i].at[block],
            send_sem=send_sem.at[i, k], recv_sem=recv_sem.at[i, k],
            device_id={"ep": to}, device_id_type=MESH)

    for e in range(n_local):
        for k in range(3):
            w_copy(k, e).start(priority=1)
    for c in loads:
        c.wait()
    pl.semaphore_wait(barrier, 3)
    to_opp = [send(i, me, opp, 0) for i in range(5)]
    to_sib = [send(i, me, sib, 1) for i in range(5)]
    relay = [send(i, opp, sib, 2) for i in range(4)] + [send(4, me, diag, 2)]
    for i in range(5):
        to_opp[i].start()
        to_sib[i].start()
    relay[4].start()
    def ready(e):
        for k in range(3):
            w_copy(k, e).wait()

    def flip(e):
        if FLIP2:
            w2T[e % TURNS] = w2[e].T
        if FLIP1:
            w1T[e % TURNS] = w1[e].T
        if FLIP3:
            w3T[e % TURNS] = w3[e].T

    def flips(lo, hi):
        for e in range(lo, hi):
            ready(e)
            flip(e)

    flips(0, CUTS[0])
    for i in range(3):
        to_opp[i].wait_recv()
        relay[i].start()
    flips(CUTS[0], CUTS[1])
    to_opp[3].wait_recv()
    relay[3].start()
    for i in range(3):
        to_sib[i].wait_recv()
        relay[i].wait_recv()

    def rows_of(buf):
        return jnp.concatenate([buf[b] for b in range(n)], axis=1).T

    lane = lax.broadcasted_iota(jnp.int32, (n_tok, LANE), 1)
    ib, gt, sl = rows_of(idx_v), rows_of(gate_v), rows_of(slot_v)
    gd = jnp.zeros((n_tok, LANE), F32)
    md = jnp.zeros((n_tok, LANE), F32)
    for j in range(ib.shape[1]):
        hit = (ib[:, j:j + 1] == lane + me * n_local) & (sl[:, j:j + 1] >= 0)
        gd = jnp.where(hit, gt[:, j:j + 1], gd)
        md = jnp.where(hit, 1.0, md)
    for e in range(n_local):
        gb[e] = jnp.broadcast_to(gd[:, e:e + 1], (n_tok, LANE))
        mb[e] = jnp.broadcast_to(md[:, e:e + 1], (n_tok, LANE))


    half = 256

    def rows(block):
        return pl.ds(pl.multiple_of(block * tok, tok), tok)

    spans = (pl.ds(0, wide), pl.ds(wide, model))

    def swap(k, b):
        block = (diag, sib)[b]
        return pltpu.make_async_remote_copy(
            src_ref=acc.at[rows(block), spans[k]], dst_ref=inbox.at[b, :, spans[k]],
            send_sem=part_send.at[k, b], recv_sem=part_recv.at[k, b],
            device_id={"ep": sib}, device_id_type=MESH)

    def start_swap(k):
        for b in range(2):
            swap(k, b).start()

    def keep_of(e):
        keep = mb[e] > 0.0
        return jnp.concatenate([keep, keep], axis=1)

    def up(e, c):
        col = slice(c * half, (c + 1) * half)
        xv = xg[...].reshape(n_tok, model)
        keep = keep_of(e)
        a = jnp.where(keep, dot(xv, w1[e, :, col]), 0.0)
        b = jnp.where(keep, dot(xv, w3[e, :, col]), 0.0)
        sg = jax.nn.sigmoid(a)
        ga = a * sg
        h = (ga * b).astype(BF16)
        h_v[e, :, col] = h
        hT[e, col, :] = h.T
        return b * (sg * (1.0 + a * (1.0 - sg))), ga

    def add(e, col, val):
        acc[:, col] = val if e == 0 else acc[:, col] + val

    def expert(e):
        gv = gb[e]
        if e == 5:
            xT[...] = xg[...].reshape(n_tok, model).T
        for c in range(model // LANE):
            col = slice(c * LANE, (c + 1) * LANE)
            dy[e, :, col] = (gv * gg[:, :, col].reshape(n_tok, LANE).astype(F32)).astype(BF16)
        for c in range(ffn // half):
            col = slice(c * half, (c + 1) * half)
            pre, ga = (pf[e, :, col], qf[e, :, col]) if e < EARLY else up(e, c)
            dh = dot(dy[e], w2T[e % TURNS, :, col]) if FLIP2 else dot_nt(dy[e], w2[e, col, :])
            da[e, :, col] = (dh * pre).astype(BF16)
            db[e, :, col] = (dh * ga).astype(BF16)
        if e + CUTS[2] < n_local:
            flip(e + CUTS[2])
        part = jnp.zeros((n_tok, LANE), F32)
        for c in range(model // half):
            y = dot(h_v[e], w2[e, :, c * half:(c + 1) * half]).astype(BF16).astype(F32)
            for k in range(half // LANE):
                yk = y[:, k * LANE:(k + 1) * LANE]
                col = slice(c * half + k * LANE, c * half + (k + 1) * LANE)
                add(e, col, gv * yk)
                part += gg[:, :, col].reshape(n_tok, LANE).astype(F32) * yk
        row = jnp.sum(part, axis=1, keepdims=True)
        add(e, slice(model, wide), jnp.where(lane == me * n_local + e, row, 0.0))
        if e + 1 == n_local:
            start_swap(0)
        for c in range(model // half):
            col = slice(c * half, (c + 1) * half)
            both = jnp.concatenate([da[e], db[e]], axis=1)
            dr = dot(both, jnp.concatenate([w1T[e % TURNS, :, col], w3T[e % TURNS, :, col]], axis=0))
            add(e, slice(wide + c * half, wide + (c + 1) * half), dr.astype(BF16).astype(F32))

    flips(CUTS[1], CUTS[2])
    for e in range(CUTS[2], EARLY):
        ready(e)
    to_sib[3].wait_recv()
    relay[3].wait_recv()
    for e in range(EARLY):
        for c in range(ffn // half):
            col = slice(c * half, (c + 1) * half)
            pf[e, :, col], qf[e, :, col] = up(e, c)
    to_opp[4].wait_recv()
    to_sib[4].wait_recv()
    relay[4].wait_recv()
    for e0 in range(0, n_local, unroll):
        for e in range(max(EARLY, CUTS[2], e0 + CUTS[2] if e0 else 0), min(e0 + unroll + CUTS[2], n_local)):
            ready(e)
        for e in range(e0, e0 + unroll):
            expert(e)

    start_swap(1)
    for k, col in enumerate(spans):
        swap(k, 0).wait_recv()
        out_send[:, col] = acc[rows(opp), col] + inbox[0, :, col]
        swap(k, 1).wait_recv()
        own[:, col] = acc[rows(me), col] + inbox[1, :, col]
    for k in range(2):
        for b in range(2):
            swap(k, b).wait_send()
    for i in range(5):
        to_opp[i].wait_send()
        to_sib[i].wait_send()
        relay[i].wait_send()


def wgrad_kernel(xT, hT, dy, da, db, g1_h, g3_h, g2_h, st1, st3, st2, sem):
    n_local = da.shape[0]
    half = 256

    def copy(k, e):
        st, gh = ((st2, g2_h), (st1, g1_h), (st3, g3_h))[k]
        return pltpu.make_async_copy(st.at[e], gh.at[e], sem.at[k, e])

    def body(e, _):
        for c in range(dy.shape[2] // half):
            col = slice(c * half, (c + 1) * half)
            st2[e, :, col] = dot(hT[e], dy[e, :, col]).astype(BF16)
        copy(0, e).start()
        for k, st, src in ((1, st1, da), (2, st3, db)):
            for c in range(da.shape[2] // half):
                col = slice(c * half, (c + 1) * half)
                st[e, :, col] = dot(xT[...], src[e, :, col]).astype(BF16)
            copy(k, e).start()
        return 0

    lax.fori_loop(0, n_local, body, 0, unroll=2)
    for e in range(n_local):
        for k in range(3):
            copy(k, e).wait()


def final_kernel(idx, slot, own, got, out, gx, ggate):
    model = out.shape[1]
    wide = model + LANE
    out[...] = (own[:, :model] + got[:, :model]).astype(BF16)
    gx[...] = (own[:, wide:] + got[:, wide:]).astype(BF16)
    dense = (own[:, model:wide] + got[:, model:wide]).T
    expert = lax.broadcasted_iota(jnp.int32, dense.shape, 0)
    for j in range(idx.shape[0]):
        hit = (expert == idx[j:j + 1, :]) & (slot[j:j + 1, :] >= 0)
        ggate[j:j + 1, :] = jnp.sum(jnp.where(hit, dense, 0.0), axis=0, keepdims=True)


def vm(shape, dtype):
    return pltpu.VMEM(shape, dtype)


def in_vmem(x):
    return pltpu.with_memory_space_constraint(x, pltpu.VMEM)


def in_hbm(x):
    return pltpu.with_memory_space_constraint(x, pltpu.HBM)


UNROLL = 4
EARLY = 5
CUTS = (2, 4, 4)
TURNS = 5
FLIP2 = True
FLIP1 = True
FLIP3 = True


def solution(mesh):
    n = mesh.shape["ep"]
    row_spec = P(("dp", "ep"))
    expert_spec = P("ep")
    ANY = pl.BlockSpec(memory_space=pl.ANY)
    HB = pl.BlockSpec(memory_space=pltpu.HBM)
    VM = pl.BlockSpec(memory_space=pltpu.VMEM)

    def per_device(x_rows, expert_idx, gate_w, slot_pos, w_gate, w_up, w_down, grad_out):
        tok, model = x_rows.shape
        top = expert_idx.shape[1]
        nl, _, ffn = w_gate.shape
        nt = n * tok
        S = jax.ShapeDtypeStruct
        width = 2 * model + LANE
        flops = 2 * nt * model * ffn * nl
        DMA = pltpu.SemaphoreType.DMA
        hT, dy, da, db, xT, own, opp_sum = pl.pallas_call(
            functools.partial(token_kernel, n, UNROLL),
            out_shape=(vm((nl, ffn, nt), BF16), vm((nl, nt, model), BF16), vm((nl, nt, ffn), BF16), vm((nl, nt, ffn), BF16),
                       vm((model, nt), BF16), vm((tok, width), F32), S((tok, width), F32)),
            in_specs=[HB] * 8,
            out_specs=[VM] * 7,
            scratch_shapes=[
                pltpu.VMEM(w_gate.shape, BF16), pltpu.VMEM(w_up.shape, BF16), pltpu.VMEM(w_down.shape, BF16),
                pltpu.VMEM((TURNS, model, ffn), BF16), pltpu.VMEM((TURNS, ffn, model), BF16), pltpu.VMEM((TURNS, ffn, model), BF16),
                pltpu.VMEM((n, tok, model), BF16), pltpu.VMEM((n, tok, model), BF16),
                pltpu.VMEM((n, top, tok), jnp.int32), pltpu.VMEM((n, top, tok), F32), pltpu.VMEM((n, top, tok), jnp.int32),
                pltpu.VMEM((nl, nt, LANE), F32), pltpu.VMEM((nl, nt, LANE), F32),
                pltpu.VMEM((EARLY, nt, ffn), F32), pltpu.VMEM((EARLY, nt, ffn), F32), pltpu.VMEM((nl, nt, ffn), BF16),
                pltpu.VMEM((nt, width), F32), pltpu.VMEM((2, tok, width), F32),
                DMA((5,)), DMA((3, nl)), DMA((5, 3)), DMA((5, 3)), DMA((2, 2)), DMA((2, 2)),
            ],
            compiler_params=pltpu.CompilerParams(collective_id=0, has_side_effects=True, vmem_limit_bytes=57 << 20),
            cost_estimate=pl.CostEstimate(flops=6 * flops, bytes_accessed=25 << 20, transcendentals=0),
            name="moe_tokens",
        )(*[in_hbm(v) for v in (expert_idx.T, gate_w.T, slot_pos.T, x_rows, grad_out, w_gate, w_up, w_down)])

        got = lax.ppermute(opp_sum, "ep", [(i, i ^ 2) for i in range(n)])

        gw1, gw3, gwd = pl.pallas_call(
            wgrad_kernel,
            out_shape=(S(w_gate.shape, BF16), S(w_up.shape, BF16), S(w_down.shape, BF16)),
            in_specs=[VM] * 5,
            out_specs=[ANY] * 3,
            scratch_shapes=[pltpu.VMEM(w_gate.shape, BF16), pltpu.VMEM(w_up.shape, BF16), pltpu.VMEM(w_down.shape, BF16),
                            DMA((3, nl))],
            compiler_params=pltpu.CompilerParams(vmem_limit_bytes=40 << 20),
            cost_estimate=pl.CostEstimate(flops=3 * flops, bytes_accessed=25 << 20, transcendentals=0),
            name="moe_wgrad",
        )(*[in_vmem(v) for v in (xT, hT, dy, da, db)])

        out, gx, ggate = pl.pallas_call(
            final_kernel,
            out_shape=(S((tok, model), BF16), S((tok, model), BF16), S((top, tok), F32)),
            in_specs=[VM] * 4,
            out_specs=[VM] * 3,
            compiler_params=pltpu.CompilerParams(vmem_limit_bytes=8 << 20),
            name="moe_final",
        )(expert_idx.T, slot_pos.T, in_vmem(own), got)
        return out, gx, gw1, gw3, gwd, ggate.T

    return jax.shard_map(per_device, mesh=mesh,
                         in_specs=(row_spec, row_spec, row_spec, row_spec, expert_spec, expert_spec, expert_spec, row_spec),
                         out_specs=(row_spec, row_spec, row_spec, row_spec, row_spec, row_spec),
                         check_vma=False)
```

```python
import functools

import jax
import jax.numpy as jnp
from jax import lax
from jax.experimental import pallas as pl
from jax.experimental.pallas import tpu as pltpu
from jax.sharding import PartitionSpec as P

F32 = jnp.float32
BF16 = jnp.bfloat16
MESH = pl.DeviceIdType.MESH
LANE = 128
NT = (((1,), (1,)), ((), ()))


def dot(a, b):
    return jnp.dot(a, b, preferred_element_type=F32)


def dot_nt(a, b):
    return lax.dot_general(a, b, NT, preferred_element_type=F32)


def token_kernel(n, unroll, idx_h, gate_h, slot_h, x_h, g_h, w1_h, w3_h, w2_h,
                 hT, dy, da, db, xT, own, out_send,
                 w1, w3, w2, w2T, w1T, w3T, xg, gg, idx_v, gate_v, slot_v, gb, mb, pf, qf, h_v, acc, inbox,
                 load_sem, w_sem, send_sem, recv_sem, part_send, part_recv):
    me = lax.axis_index("ep")
    sib, opp = lax.bitwise_xor(me, 1), lax.bitwise_xor(me, 2)
    diag = lax.bitwise_xor(me, 3)
    n_local = w1.shape[0]
    tok, model = x_h.shape
    ffn = w1.shape[2]
    n_tok = n * tok
    wide = model + LANE

    barrier = pltpu.get_barrier_semaphore()
    for other in (sib, opp, diag):
        pl.semaphore_signal(barrier, inc=1, device_id={"ep": other}, device_id_type=MESH)

    srcs = (idx_h, gate_h, slot_h, x_h, g_h)
    bufs = (idx_v, gate_v, slot_v, xg, gg)
    loads = [pltpu.make_async_copy(s, b.at[me], load_sem.at[i]) for i, (s, b) in enumerate(zip(srcs, bufs))]
    for c in loads:
        c.start()

    def w_copy(k, e):
        wh, wv = ((w1_h, w1), (w3_h, w3), (w2_h, w2))[k]
        return pltpu.make_async_copy(wh.at[e], wv.at[e], w_sem.at[k, e])

    def send(i, block, to, k):
        return pltpu.make_async_remote_copy(
            src_ref=bufs[i].at[block], dst_ref=bufs[i].at[block],
            send_sem=send_sem.at[i, k], recv_sem=recv_sem.at[i, k],
            device_id={"ep": to}, device_id_type=MESH)

    for e in range(n_local):
        for k in range(3):
            w_copy(k, e).start(priority=1)
    for c in loads:
        c.wait()
    pl.semaphore_wait(barrier, 3)
    to_opp = [send(i, me, opp, 0) for i in range(5)]
    to_sib = [send(i, me, sib, 1) for i in range(5)]
    relay = [send(i, opp, sib, 2) for i in range(4)] + [send(4, me, diag, 2)]
    for i in range(5):
        to_opp[i].start()
        to_sib[i].start()
    relay[4].start()
    def ready(e):
        for k in range(3):
            w_copy(k, e).wait()

    def flip(e):
        if FLIP2:
            w2T[e % TURNS] = w2[e].T
        if FLIP1:
            w1T[e % TURNS] = w1[e].T
        if FLIP3:
            w3T[e % TURNS] = w3[e].T

    def flips(lo, hi):
        for e in range(lo, hi):
            ready(e)
            flip(e)

    flips(0, CUTS[0])
    for i in range(3):
        to_opp[i].wait_recv()
        relay[i].start()
    flips(CUTS[0], CUTS[1])
    to_opp[3].wait_recv()
    relay[3].start()
    for i in range(3):
        to_sib[i].wait_recv()
        relay[i].wait_recv()

    def rows_of(buf):
        return jnp.concatenate([buf[b] for b in range(n)], axis=1).T

    lane = lax.broadcasted_iota(jnp.int32, (n_tok, LANE), 1)
    ib, gt, sl = rows_of(idx_v), rows_of(gate_v), rows_of(slot_v)
    gd = jnp.zeros((n_tok, LANE), F32)
    md = jnp.zeros((n_tok, LANE), F32)
    for j in range(ib.shape[1]):
        hit = (ib[:, j:j + 1] == lane + me * n_local) & (sl[:, j:j + 1] >= 0)
        gd = jnp.where(hit, gt[:, j:j + 1], gd)
        md = jnp.where(hit, 1.0, md)
    for e in range(n_local):
        gb[e] = jnp.broadcast_to(gd[:, e:e + 1], (n_tok, LANE))
        mb[e] = jnp.broadcast_to(md[:, e:e + 1], (n_tok, LANE))


    half = 256

    def rows(block):
        return pl.ds(pl.multiple_of(block * tok, tok), tok)

    spans = (pl.ds(0, wide), pl.ds(wide, model))

    def swap(k, b):
        block = (diag, sib)[b]
        return pltpu.make_async_remote_copy(
            src_ref=acc.at[rows(block), spans[k]], dst_ref=inbox.at[b, :, spans[k]],
            send_sem=part_send.at[k, b], recv_sem=part_recv.at[k, b],
            device_id={"ep": sib}, device_id_type=MESH)

    def start_swap(k):
        for b in range(2):
            swap(k, b).start()

    def keep_of(e):
        keep = mb[e] > 0.0
        return jnp.concatenate([keep, keep], axis=1)

    def up(e, c):
        col = slice(c * half, (c + 1) * half)
        xv = xg[...].reshape(n_tok, model)
        keep = keep_of(e)
        a = jnp.where(keep, dot(xv, w1[e, :, col]), 0.0)
        b = jnp.where(keep, dot(xv, w3[e, :, col]), 0.0)
        sg = jax.nn.sigmoid(a)
        ga = a * sg
        h = (ga * b).astype(BF16)
        h_v[e, :, col] = h
        hT[e, col, :] = h.T
        return b * (sg * (1.0 + a * (1.0 - sg))), ga

    def add(e, col, val):
        acc[:, col] = val if e == 0 else acc[:, col] + val

    def expert(e):
        gv = gb[e]
        if e == 5:
            xT[...] = xg[...].reshape(n_tok, model).T
        for c in range(model // LANE):
            col = slice(c * LANE, (c + 1) * LANE)
            dy[e, :, col] = (gv * gg[:, :, col].reshape(n_tok, LANE).astype(F32)).astype(BF16)
        for c in range(ffn // half):
            col = slice(c * half, (c + 1) * half)
            pre, ga = (pf[e, :, col], qf[e, :, col]) if e < EARLY else up(e, c)
            dh = dot(dy[e], w2T[e % TURNS, :, col]) if FLIP2 else dot_nt(dy[e], w2[e, col, :])
            da[e, :, col] = (dh * pre).astype(BF16)
            db[e, :, col] = (dh * ga).astype(BF16)
        if e + CUTS[2] < n_local:
            flip(e + CUTS[2])
        part = jnp.zeros((n_tok, LANE), F32)
        for c in range(model // half):
            y = dot(h_v[e], w2[e, :, c * half:(c + 1) * half]).astype(BF16).astype(F32)
            for k in range(half // LANE):
                yk = y[:, k * LANE:(k + 1) * LANE]
                col = slice(c * half + k * LANE, c * half + (k + 1) * LANE)
                add(e, col, gv * yk)
                part += gg[:, :, col].reshape(n_tok, LANE).astype(F32) * yk
        row = jnp.sum(part, axis=1, keepdims=True)
        add(e, slice(model, wide), jnp.where(lane == me * n_local + e, row, 0.0))
        if e + 1 == n_local:
            start_swap(0)
        for c in range(model // half):
            col = slice(c * half, (c + 1) * half)
            both = jnp.concatenate([da[e], db[e]], axis=1)
            dr = dot(both, jnp.concatenate([w1T[e % TURNS, :, col], w3T[e % TURNS, :, col]], axis=0))
            add(e, slice(wide + c * half, wide + (c + 1) * half), dr.astype(BF16).astype(F32))

    flips(CUTS[1], CUTS[2])
    for e in range(CUTS[2], EARLY):
        ready(e)
    to_sib[3].wait_recv()
    relay[3].wait_recv()
    for e in range(EARLY):
        for c in range(ffn // half):
            col = slice(c * half, (c + 1) * half)
            pf[e, :, col], qf[e, :, col] = up(e, c)
    to_opp[4].wait_recv()
    to_sib[4].wait_recv()
    relay[4].wait_recv()
    for e0 in range(0, n_local, unroll):
        for e in range(max(EARLY, CUTS[2], e0 + CUTS[2] if e0 else 0), min(e0 + unroll + CUTS[2], n_local)):
            ready(e)
        for e in range(e0, e0 + unroll):
            expert(e)

    start_swap(1)
    for k, col in enumerate(spans):
        swap(k, 0).wait_recv()
        out_send[:, col] = acc[rows(opp), col] + inbox[0, :, col]
        swap(k, 1).wait_recv()
        own[:, col] = acc[rows(me), col] + inbox[1, :, col]
    for k in range(2):
        for b in range(2):
            swap(k, b).wait_send()
    for i in range(5):
        to_opp[i].wait_send()
        to_sib[i].wait_send()
        relay[i].wait_send()


def wgrad_kernel(xT, hT, dy, da, db, g1_h, g3_h, g2_h, st1, st3, st2, sem):
    n_local = da.shape[0]
    half = 256

    def copy(k, e):
        st, gh = ((st2, g2_h), (st1, g1_h), (st3, g3_h))[k]
        return pltpu.make_async_copy(st.at[e], gh.at[e], sem.at[k, e])

    def body(e, _):
        for c in range(dy.shape[2] // half):
            col = slice(c * half, (c + 1) * half)
            st2[e, :, col] = dot(hT[e], dy[e, :, col]).astype(BF16)
        copy(0, e).start()
        for k, st, src in ((1, st1, da), (2, st3, db)):
            for c in range(da.shape[2] // half):
                col = slice(c * half, (c + 1) * half)
                st[e, :, col] = dot(xT[...], src[e, :, col]).astype(BF16)
            copy(k, e).start()
        return 0

    lax.fori_loop(0, n_local, body, 0, unroll=2)
    for e in range(n_local):
        for k in range(3):
            copy(k, e).wait()


def final_kernel(idx, slot, own, got, out, gx, ggate):
    model = out.shape[1]
    wide = model + LANE
    out[...] = (own[:, :model] + got[:, :model]).astype(BF16)
    gx[...] = (own[:, wide:] + got[:, wide:]).astype(BF16)
    dense = (own[:, model:wide] + got[:, model:wide]).T
    expert = lax.broadcasted_iota(jnp.int32, dense.shape, 0)
    for j in range(idx.shape[0]):
        hit = (expert == idx[j:j + 1, :]) & (slot[j:j + 1, :] >= 0)
        ggate[j:j + 1, :] = jnp.sum(jnp.where(hit, dense, 0.0), axis=0, keepdims=True)


def vm(shape, dtype):
    return pltpu.VMEM(shape, dtype)


def in_vmem(x):
    return pltpu.with_memory_space_constraint(x, pltpu.VMEM)


def in_hbm(x):
    return pltpu.with_memory_space_constraint(x, pltpu.HBM)


UNROLL = 4
EARLY = 5
CUTS = (2, 4, 4)
TURNS = 6
FLIP2 = True
FLIP1 = True
FLIP3 = True


def solution(mesh):
    n = mesh.shape["ep"]
    row_spec = P(("dp", "ep"))
    expert_spec = P("ep")
    ANY = pl.BlockSpec(memory_space=pl.ANY)
    HB = pl.BlockSpec(memory_space=pltpu.HBM)
    VM = pl.BlockSpec(memory_space=pltpu.VMEM)

    def per_device(x_rows, expert_idx, gate_w, slot_pos, w_gate, w_up, w_down, grad_out):
        tok, model = x_rows.shape
        top = expert_idx.shape[1]
        nl, _, ffn = w_gate.shape
        nt = n * tok
        S = jax.ShapeDtypeStruct
        width = 2 * model + LANE
        flops = 2 * nt * model * ffn * nl
        DMA = pltpu.SemaphoreType.DMA
        hT, dy, da, db, xT, own, opp_sum = pl.pallas_call(
            functools.partial(token_kernel, n, UNROLL),
            out_shape=(vm((nl, ffn, nt), BF16), vm((nl, nt, model), BF16), vm((nl, nt, ffn), BF16), vm((nl, nt, ffn), BF16),
                       vm((model, nt), BF16), vm((tok, width), F32), S((tok, width), F32)),
            in_specs=[HB] * 8,
            out_specs=[VM] * 7,
            scratch_shapes=[
                pltpu.VMEM(w_gate.shape, BF16), pltpu.VMEM(w_up.shape, BF16), pltpu.VMEM(w_down.shape, BF16),
                pltpu.VMEM((TURNS, model, ffn), BF16), pltpu.VMEM((TURNS, ffn, model), BF16), pltpu.VMEM((TURNS, ffn, model), BF16),
                pltpu.VMEM((n, tok, model), BF16), pltpu.VMEM((n, tok, model), BF16),
                pltpu.VMEM((n, top, tok), jnp.int32), pltpu.VMEM((n, top, tok), F32), pltpu.VMEM((n, top, tok), jnp.int32),
                pltpu.VMEM((nl, nt, LANE), F32), pltpu.VMEM((nl, nt, LANE), F32),
                pltpu.VMEM((EARLY, nt, ffn), F32), pltpu.VMEM((EARLY, nt, ffn), F32), pltpu.VMEM((nl, nt, ffn), BF16),
                pltpu.VMEM((nt, width), F32), pltpu.VMEM((2, tok, width), F32),
                DMA((5,)), DMA((3, nl)), DMA((5, 3)), DMA((5, 3)), DMA((2, 2)), DMA((2, 2)),
            ],
            compiler_params=pltpu.CompilerParams(collective_id=0, has_side_effects=True, vmem_limit_bytes=57 << 20),
            cost_estimate=pl.CostEstimate(flops=6 * flops, bytes_accessed=25 << 20, transcendentals=0),
            name="moe_tokens",
        )(*[in_hbm(v) for v in (expert_idx.T, gate_w.T, slot_pos.T, x_rows, grad_out, w_gate, w_up, w_down)])

        got = lax.ppermute(opp_sum, "ep", [(i, i ^ 2) for i in range(n)])

        gw1, gw3, gwd = pl.pallas_call(
            wgrad_kernel,
            out_shape=(S(w_gate.shape, BF16), S(w_up.shape, BF16), S(w_down.shape, BF16)),
            in_specs=[VM] * 5,
            out_specs=[ANY] * 3,
            scratch_shapes=[pltpu.VMEM(w_gate.shape, BF16), pltpu.VMEM(w_up.shape, BF16), pltpu.VMEM(w_down.shape, BF16),
                            DMA((3, nl))],
            compiler_params=pltpu.CompilerParams(vmem_limit_bytes=40 << 20),
            cost_estimate=pl.CostEstimate(flops=3 * flops, bytes_accessed=25 << 20, transcendentals=0),
            name="moe_wgrad",
        )(*[in_vmem(v) for v in (xT, hT, dy, da, db)])

        out, gx, ggate = pl.pallas_call(
            final_kernel,
            out_shape=(S((tok, model), BF16), S((tok, model), BF16), S((top, tok), F32)),
            in_specs=[VM] * 4,
            out_specs=[VM] * 3,
            compiler_params=pltpu.CompilerParams(vmem_limit_bytes=8 << 20),
            name="moe_final",
        )(expert_idx.T, slot_pos.T, in_vmem(own), got)
        return out, gx, gw1, gw3, gwd, ggate.T

    return jax.shard_map(per_device, mesh=mesh,
                         in_specs=(row_spec, row_spec, row_spec, row_spec, expert_spec, expert_spec, expert_spec, row_spec),
                         out_specs=(row_spec, row_spec, row_spec, row_spec, row_spec, row_spec),
                         check_vma=False)
```
